32 devices in a mesh: group: 8 (over y, x, core), ep: 4 (over z).
Axes of the slice: x: 2, y: 2, z: 4, core: 2. Of those that a mesh axis runs over, the one named last changes fastest.
Arguments:
- tokens: bfloat16 [1024, 3584], P(('group', 'ep')), may hold values from -6 to 6
- expert_ids: int32 [1024, 8], P(('group', 'ep')), may hold values from 0 to 31, as said below
- gate_scores: float32 [1024, 8], P(('group', 'ep')), may hold values from 0.05 to 0.35
- replica_pick: int32 [1024, 8], P(('group', 'ep')), may hold values from 0 to 8
- replica_hot: int32 [4], replicated, may hold values from 0 to 7
- gate_weight: bfloat16 [32, 3584, 1024], P(('group', 'ep')), may hold values from -0.09375 to 0.09375
- up_weight: bfloat16 [32, 3584, 1024], P(('group', 'ep')), may hold values from -0.09375 to 0.09375
- down_weight: bfloat16 [32, 1024, 3584], P(('group', 'ep')), may hold values from -0.1875 to 0.1875
Outputs:
- mixed: bfloat16 [1024, 3584], P(('group', 'ep'))
- slot_load: float32 [32, 2], P(('group', 'ep'))
The draws below stay inside these ranges and needn't reach their ends.
Inputs may be any that keep to these rules, and one draw needn't show every extreme that they name: `expert_ids`: each row names 8 different experts; in each aligned block of 16 rows (one micro-batch of one device) no expert is named by more than 5 rows, and the expert replica_hot[c] * 4 + c of each ep index c is named by exactly 5 rows.
All inputs are finite; a program needn't handle non-finite values.
Results may differ from the reference program's by a relative error of at most 0.0057.
Values may be sent and summed in bfloat16 or wider, within the bound.
A program may use at most 128 MiB of HBM per device.

```python
import jax
import jax.numpy as jnp
from jax import lax

D = 3584
FF = 1024
TOP = 8
MICRO = 2
MB_TOK = 16
EXPERTS = 32
TOKENS = 1024
MOST = 5
N_GROUP = 8
N_EP = 4


def hot_groups(key):
    base = jax.random.randint(jax.random.fold_in(key, 7), (N_EP,), 0, N_GROUP).astype(jnp.int32)
    where_top = jax.random.randint(jax.random.fold_in(key, 8), (), 0, N_EP).astype(jnp.int32)
    where_low = (where_top + 1) % N_EP
    base = base.at[where_top].set(N_GROUP - 1)
    base = base.at[where_low].set(0)
    return base.astype(jnp.int32)


def draw_replica_hot(key, part):
    return hot_groups(key)


def draw_expert_ids(key, part):
    hot_group = hot_groups(key)
    expert_range = jnp.arange(EXPERTS, dtype=jnp.int32)
    not_hot = 1 - (hot_group[expert_range % N_EP] == expert_range // N_EP).astype(jnp.int32)
    hot_pairs = N_EP * MOST
    rest_pairs = max(MB_TOK * TOP - hot_pairs, 1)
    rest_count = EXPERTS - N_EP
    row_index = jnp.arange(MB_TOK, dtype=jnp.int32)[:, None]
    col_index = jnp.arange(TOP, dtype=jnp.int32)[None, :]
    pair_index = col_index * MB_TOK + row_index
    rest_index = N_EP + jnp.maximum(pair_index - hot_pairs, 0) * rest_count // rest_pairs
    place = jnp.where(pair_index < hot_pairs, pair_index // MOST, rest_index).astype(jnp.int32)

    def one_block(block):
        shuffle = jax.random.permutation(jax.random.fold_in(key, 1000 + block), EXPERTS).astype(jnp.int32)
        ordering = shuffle[jnp.argsort(not_hot[shuffle], stable=True)]
        return ordering[place]
    blocks = jax.vmap(one_block)(jnp.arange(TOKENS // MB_TOK, dtype=jnp.int32))
    return blocks.reshape(TOKENS, TOP).astype(jnp.int32)


def with_ends(array, rng, least, largest):
    dims = array.shape
    spot = [jax.random.randint(jax.random.fold_in(rng, axis), (), 0, dims[axis]) for axis in range(len(dims))]
    array = array.at[tuple(spot)].set(least)
    longest = dims.index(max(dims))
    spot[longest] = (spot[longest] + 1) % dims[longest]
    return array.at[tuple(spot)].set(largest)


def levels(rng, dims, pieces, smallest, high):
    def one(dim, parts):
        draws = jax.random.uniform(jax.random.fold_in(jax.random.fold_in(rng, 6), dim), (parts,), jnp.float32, smallest / len(pieces), high / len(pieces))
        return jnp.repeat(jnp.exp(draws), dims[dim] // parts).reshape((-1,) + (1,) * (len(dims) - dim - 1))

    loudness = one(*pieces[0])
    for cut in pieces[1:]:
        loudness = loudness * one(*cut)
    return loudness


def bell_draw(own_key, shape, deviation, most, shards=(), held_as=jnp.bfloat16):
    result = jax.random.normal(own_key, shape, jnp.float32) * deviation
    if len(shards) > 0:
        result = levels(own_key, shape, shards, -0.22, 0.18) * result
    return jnp.clip(result, min=-most, max=most).astype(held_as)


def setup_inputs(seed: int = 0) -> dict:
    splits = jax.random.split(jax.random.key(seed), 9)
    tokens = bell_draw(splits[0], (TOKENS, D), 1.0, 6.0, ((0, 32),))
    expert_ids = draw_expert_ids(jax.random.fold_in(splits[8], 71), 0)
    gate_scores = jnp.clip(0.05 + 0.29999999 * jax.random.uniform(splits[2], (TOKENS, TOP), jnp.float32) ** levels(splits[2], (TOKENS, TOP), ((0, 32),), -0.2, 0.2), 0.05, 0.35)
    replica_pick = with_ends(jax.random.randint(splits[3], (TOKENS, TOP), 0, N_GROUP + 1), jax.random.fold_in(splits[3], 1), 0, N_GROUP).astype(jnp.int32)
    replica_hot = draw_replica_hot(jax.random.fold_in(splits[8], 71), 0)
    gate_weight = bell_draw(splits[5], (EXPERTS, D, FF), D ** -0.5, 0.09375, ((0, 32),))
    up_weight = bell_draw(splits[6], (EXPERTS, D, FF), D ** -0.5, 0.09375, ((0, 32),))
    down_weight = bell_draw(splits[7], (EXPERTS, FF, D), FF ** -0.5, 0.1875, ((0, 32),))
    return {"tokens": tokens, "expert_ids": expert_ids, "gate_scores": gate_scores, "replica_pick": replica_pick, "replica_hot": replica_hot, "gate_weight": gate_weight, "up_weight": up_weight, "down_weight": down_weight}


def expert_ffn(inputs, w_gate, w_up, w_down):
    gate_act = jnp.dot(inputs, w_gate, preferred_element_type=jnp.float32)
    up_act = jnp.dot(inputs, w_up, preferred_element_type=jnp.float32)
    hidden = (jax.nn.silu(gate_act) * up_act).astype(jnp.bfloat16)
    return jnp.dot(hidden, w_down, preferred_element_type=jnp.float32).astype(jnp.bfloat16)


def reference(tokens, expert_ids, gate_scores, replica_pick, replica_hot, gate_weight, up_weight, down_weight):
    flat_ids = expert_ids.reshape(-1).astype(jnp.int32)
    pair_count = flat_ids.shape[0]
    sort_order = jnp.argsort(flat_ids, stable=True).astype(jnp.int32)
    counts = jnp.zeros((EXPERTS,), jnp.int32).at[flat_ids].add(1)
    starts = (jnp.cumsum(counts) - counts).astype(jnp.int32)
    inverse = jnp.zeros((pair_count,), jnp.int32).at[sort_order].set(jnp.arange(pair_count, dtype=jnp.int32))
    pair_rank = (inverse - starts[flat_ids]).astype(jnp.int32)
    capacity = MICRO * MOST * EXPERTS
    sorted_tokens = jnp.concatenate([(sort_order // TOP).astype(jnp.int32), jnp.zeros((capacity,), jnp.int32)])

    def one_expert(expert):
        token_index = lax.dynamic_slice_in_dim(sorted_tokens, starts[expert], capacity)
        return expert_ffn(tokens[token_index], gate_weight[expert], up_weight[expert], down_weight[expert])

    expert_outs = lax.map(one_expert, jnp.arange(EXPERTS, dtype=jnp.int32))
    pair_outs = expert_outs[flat_ids, pair_rank].reshape(TOKENS, TOP, D).astype(jnp.float32)
    mixed = jnp.sum(gate_scores[:, :, None] * pair_outs, axis=1).astype(jnp.bfloat16)

    column = flat_ids % N_EP
    home_group = flat_ids // N_EP
    pick_flat = replica_pick.reshape(-1).astype(jnp.int32)
    replicated = (replica_hot[column] == home_group) & (pick_flat < N_GROUP)
    device = jnp.where(replicated, pick_flat, home_group) * N_EP + column
    slot_key = (device * 2 + replicated.astype(jnp.int32)).astype(jnp.int32)
    slot_load = jnp.zeros((2 * EXPERTS,), jnp.float32).at[slot_key].add(1.0).reshape(EXPERTS, 2) / TOP
    return mixed, slot_load
```

```python
import functools
import math

import jax
import jax.numpy as jnp
from jax import lax
from jax.experimental import pallas as pl
from jax.experimental.pallas import tpu as pltpu
from jax.sharding import PartitionSpec as P

AXES = ("group", "ep")
MESH = pl.DeviceIdType.MESH

LINE_STEP, RING_STEP, DEEP_STEP, PRODUCT_STEP = 1.1, 3.1, 2.3, 2.6
SPREAD_STEP, BACK_RING, BACK_LINE, BACK_DEEP = 2.0, 2.0, 2.0, 2.0
PIECES = 2
INTO = (("line", 4, 5.0), ("line", 4, 0.0), ("line", 3, 0.0), ("ring", 3, 0.0))
OUTOF = (("ring", 3, 0.0), ("line", 4, 1.0), ("line", 4, 4.0), ("line", 3, 8.0))
VMEM_LIMIT = 67043328


def place_of(nplane, nep):
    group = lax.axis_index("group")
    ep = lax.axis_index("ep")
    core = lax.rem(group, 2)
    plane = lax.div(group, 2)

    def plane_peer(step):
        other = lax.rem(plane + step, nplane)
        return other, (other * 2 + core, ep)

    def ep_peer(step):
        other = lax.rem(ep + step, nep)
        return other, (group, other)

    return plane, ep, plane_peer, ep_peer


def greet(nplane, nep, plane_peer, ep_peer):
    barrier = pltpu.get_barrier_semaphore()
    for step in range(1, nplane):
        pl.semaphore_signal(barrier, inc=1, device_id=plane_peer(step)[1], device_id_type=MESH)
    for step in range(1, nep):
        pl.semaphore_signal(barrier, inc=1, device_id=ep_peer(step)[1], device_id_type=MESH)
    pl.semaphore_wait(barrier, nplane + nep - 2)


def gather_kernel(
    nplane, nep, cut, x_ref, note_ref, out_ref, notes_ref,
    own_sem, send_a, recv_a, send_b, recv_b, right_a, left_a, right_b, left_b, note_send, note_recv,
):
    plane, ep, plane_peer, ep_peer = place_of(nplane, nep)
    group = lax.axis_index("group")
    me = group * nep + ep
    total = 2 * nplane * nep
    width = x_ref.shape[1]
    cols = {"a": pl.ds(0, cut), "b": pl.ds(cut, width - cut)}
    recv = {"a": recv_a, "b": recv_b}
    rights = {"a": right_a, "b": right_b}
    lefts = {"a": left_a, "b": left_b}
    own = pltpu.make_async_copy(x_ref, out_ref.at[plane, ep], own_sem.at[0])
    own.start()
    own_note = pltpu.make_async_copy(note_ref, notes_ref.at[me], own_sem.at[1])
    own_note.start()

    barrier = pltpu.get_barrier_semaphore()
    for step in range(1, total):
        other = lax.rem(me + step, total)
        pl.semaphore_signal(
            barrier, inc=1, device_id=(lax.div(other, nep), lax.rem(other, nep)), device_id_type=MESH
        )
    pl.semaphore_wait(barrier, total - 1)

    def copy(src, p, e, half, send, target):
        return pltpu.make_async_remote_copy(
            src_ref=src.at[:, cols[half]],
            dst_ref=out_ref.at[p, e, :, cols[half]],
            send_sem=send,
            recv_sem=recv[half].at[p * nep + e],
            device_id=target,
            device_id_type=MESH,
        )

    sends = []
    used = {"a": 0, "b": 0}

    def push(src, p, e, half):
        send = send_a if half == "a" else send_b
        for step in range(1, nplane):
            made = copy(src, p, e, half, send.at[used[half]], plane_peer(step)[1])
            used[half] += 1
            made.start()
            sends.append(made)

    def arrived(p, e, half):
        copy(out_ref.at[p, e], p, e, half, send_a.at[0], ep_peer(1)[1]).wait_recv()

    def to_right(src, p, e, half):
        return copy(src, p, e, half, rights[half].at[p * nep + e], (group, lax.rem(ep + 1, nep)))

    def to_left(src, p, e, half):
        return copy(src, p, e, half, lefts[half].at[p * nep + e], (group, lax.rem(ep + nep - 1, nep)))

    has_right, has_left = ep < nep - 1, ep > 0

    def both_ways(src, p, half):
        @pl.when(has_right)
        def _():
            to_right(src, p, ep, half).start()

        @pl.when(has_left)
        def _():
            to_left(src, p, ep, half).start()

    def chain(p, back, half):
        @pl.when(ep - back >= 0)
        def _():
            arrived(p, ep - back, half)

            @pl.when(has_right)
            def _():
                to_right(out_ref.at[p, ep - back], p, ep - back, half).start()

        @pl.when(ep + back < nep)
        def _():
            arrived(p, ep + back, half)

            @pl.when(has_left)
            def _():
                to_left(out_ref.at[p, ep + back], p, ep + back, half).start()

    def chain_end(p, back, half):
        @pl.when((ep - back >= 0) & has_right)
        def _():
            to_right(out_ref.at[p, ep - back], p, ep - back, half).wait_send()

        @pl.when((ep + back < nep) & has_left)
        def _():
            to_left(out_ref.at[p, ep + back], p, ep + back, half).wait_send()

    def note(source, step, target):
        return pltpu.make_async_remote_copy(
            src_ref=note_ref,
            dst_ref=notes_ref.at[source],
            send_sem=note_send.at[step],
            recv_sem=note_recv.at[source],
            device_id=(lax.div(target, nep), lax.rem(target, nep)),
            device_id_type=MESH,
        )

    both_ways(x_ref, plane, "a")
    push(x_ref, plane, ep, "b")
    push(x_ref, plane, ep, "a")
    both_ways(x_ref, plane, "b")
    for step in range(1, total):
        note(me, step, lax.rem(me + step, total)).start()
    for back in range(1, max(nplane, nep)):
        if back < nep:
            chain(plane, back, "a")
        if back < nplane:
            source = lax.rem(plane + nplane - back, nplane)
            arrived(source, ep, "b")
            both_ways(out_ref.at[source, ep], source, "b")
        if back < nep:
            left_in, right_in = ep - back >= 0, ep + back < nep

            @pl.when(left_in)
            def _():
                for step in range(1, nplane):
                    copy(
                        out_ref.at[plane, ep - back], plane, ep - back, "a",
                        send_a.at[(nplane - 1) * back + step - 1], plane_peer(step)[1],
                    ).start()

            @pl.when(right_in)
            def _():
                for step in range(1, nplane):
                    copy(
                        out_ref.at[plane, ep + back], plane, ep + back, "a",
                        send_a.at[(nplane - 1) * (nep + back) + step - 1], plane_peer(step)[1],
                    ).start()
    for back in range(1, nep):
        for p_back in range(nplane):
            chain(lax.rem(plane + nplane - p_back, nplane), back, "b")
    for p_back in range(1, nplane):
        p = lax.rem(plane + nplane - p_back, nplane)
        for e in range(nep):
            arrived(p, e, "a")
    for step in range(1, total):
        source = lax.rem(me + total - step, total)
        note(source, step, lax.rem(me + 1, total)).wait_recv()
    for made in sends:
        made.wait_send()
    for back in range(1, nep):
        @pl.when(ep - back >= 0)
        def _():
            for step in range(1, nplane):
                copy(
                    out_ref.at[plane, ep - back], plane, ep - back, "a",
                    send_a.at[(nplane - 1) * back + step - 1], plane_peer(step)[1],
                ).wait_send()

        @pl.when(ep + back < nep)
        def _():
            for step in range(1, nplane):
                copy(
                    out_ref.at[plane, ep + back], plane, ep + back, "a",
                    send_a.at[(nplane - 1) * (nep + back) + step - 1], plane_peer(step)[1],
                ).wait_send()

    for back in range(nep):
        for half in ("a", "b"):
            for p_back in range(nplane if half == "b" else 1):
                p = lax.rem(plane + nplane - p_back, nplane)
                if back == 0:
                    @pl.when(has_right)
                    def _():
                        to_right(x_ref, p, ep, half).wait_send()

                    @pl.when(has_left)
                    def _():
                        to_left(x_ref, p, ep, half).wait_send()
                else:
                    chain_end(p, back, half)
    for step in range(1, total):
        note(me, step, lax.rem(me + step, total)).wait_send()
    own.wait()
    own_note.wait()


def gather_plane(tokens, note, nplane, nep, cut):
    rows, width = tokens.shape
    count = nplane * nep
    dma = pltpu.SemaphoreType.DMA
    vmem = pl.BlockSpec(memory_space=pltpu.VMEM)
    return pl.pallas_call(
        functools.partial(gather_kernel, nplane, nep, cut),
        out_shape=[
            jax.ShapeDtypeStruct((nplane, nep, rows, width), tokens.dtype),
            jax.ShapeDtypeStruct((2 * count,) + note.shape, note.dtype),
        ],
        in_specs=[vmem, vmem],
        out_specs=[vmem, vmem],
        scratch_shapes=[
            dma((2,)),
            dma((2 * (nplane - 1) * nep,)), dma((count,)), dma((nplane - 1,)), dma((count,)),
            dma((count,)), dma((count,)), dma((count,)), dma((count,)),
            dma((2 * count,)), dma((2 * count,)),
        ],
        compiler_params=pltpu.CompilerParams(collective_id=0, has_side_effects=True),
    )(tokens, note)


def scatter_kernel(
    nplane, nep, cut, part_ref, out_ref,
    land_a1, land_b1, mid_a, mid_b, land_a2, land_b2,
    send_a1, recv_a1, send_b1, recv_b1, send_a2, recv_a2, send_b2, recv_b2,
):
    plane, ep, plane_peer, ep_peer = place_of(nplane, nep)
    width = out_ref.shape[1]
    cols_a, cols_b = pl.ds(0, cut), pl.ds(cut, width - cut)
    greet(nplane, nep, plane_peer, ep_peer)

    def move(src, dst, send, recv, target):
        made = pltpu.make_async_remote_copy(
            src_ref=src, dst_ref=dst, send_sem=send, recv_sem=recv, device_id=target, device_id_type=MESH
        )
        made.start()
        return made

    first_a, first_b = {}, {}
    for item in range(1, max(nplane, nep) + 1):
        if item <= nep:
            e = lax.rem(ep + item, nep)
            for step in range(1, nplane):
                p, target = plane_peer(step)
                spot = (step - 1) * nep + item - 1
                first_a[item, step] = move(
                    part_ref.at[p, e, :, cols_a], land_a1.at[step - 1, item - 1],
                    send_a1.at[spot], recv_a1.at[spot], target,
                )
        if item <= nplane:
            p = lax.rem(plane + item, nplane)
            for step in range(1, nep):
                e, target = ep_peer(step)
                spot = (step - 1) * nplane + item - 1
                first_b[item, step] = move(
                    part_ref.at[p, e, :, cols_b], land_b1.at[step - 1, item - 1],
                    send_b1.at[spot], recv_b1.at[spot], target,
                )
    second_a, second_b = [], []
    for item in range(1, max(nplane, nep) + 1):
        if item <= nep:
            e, target = ep_peer(item)
            total = part_ref[plane, e, :, cols_a].astype(jnp.float32)
            for step in range(1, nplane):
                first_a[item, step].wait_recv()
                total = total + land_a1[step - 1, item - 1].astype(jnp.float32)
            if item < nep:
                mid_a[item - 1] = total.astype(mid_a.dtype)
                second_a.append(
                    move(mid_a.at[item - 1], land_a2.at[item - 1], send_a2.at[item - 1], recv_a2.at[item - 1], target)
                )
            else:
                total_a = total
        if item <= nplane:
            p, target = plane_peer(item)
            total = part_ref[p, ep, :, cols_b].astype(jnp.float32)
            for step in range(1, nep):
                first_b[item, step].wait_recv()
                total = total + land_b1[step - 1, item - 1].astype(jnp.float32)
            if item < nplane:
                mid_b[item - 1] = total.astype(mid_b.dtype)
                second_b.append(
                    move(mid_b.at[item - 1], land_b2.at[item - 1], send_b2.at[item - 1], recv_b2.at[item - 1], target)
                )
            else:
                total_b = total
    for index, made in enumerate(second_a):
        made.wait_recv()
        total_a = total_a + land_a2[index].astype(jnp.float32)
    out_ref[:, cols_a] = total_a.astype(out_ref.dtype)
    for index, made in enumerate(second_b):
        made.wait_recv()
        total_b = total_b + land_b2[index].astype(jnp.float32)
    out_ref[:, cols_b] = total_b.astype(out_ref.dtype)
    for made in list(first_a.values()) + list(first_b.values()) + second_a + second_b:
        made.wait_send()


def scatter_plane(parts, cut):
    nplane, nep, rows, width = parts.shape
    rest = width - cut
    kind = parts.dtype
    dma = pltpu.SemaphoreType.DMA
    pairs_a, pairs_b = (nplane - 1) * nep, (nep - 1) * nplane
    return pl.pallas_call(
        functools.partial(scatter_kernel, nplane, nep, cut),
        out_shape=jax.ShapeDtypeStruct((rows, width), kind),
        in_specs=[pl.BlockSpec(memory_space=pltpu.VMEM)],
        out_specs=pl.BlockSpec(memory_space=pltpu.VMEM),
        scratch_shapes=[
            pltpu.VMEM((nplane - 1, nep, rows, cut), kind),
            pltpu.VMEM((nep - 1, nplane, rows, rest), kind),
            pltpu.VMEM((nep - 1, rows, cut), kind),
            pltpu.VMEM((nplane - 1, rows, rest), kind),
            pltpu.VMEM((nep - 1, rows, cut), kind),
            pltpu.VMEM((nplane - 1, rows, rest), kind),
            dma((pairs_a,)), dma((pairs_a,)), dma((pairs_b,)), dma((pairs_b,)),
            dma((nep - 1,)), dma((nep - 1,)), dma((nplane - 1,)), dma((nplane - 1,)),
        ],
        compiler_params=pltpu.CompilerParams(collective_id=1, has_side_effects=True),
    )(parts)


def ring_spot(nplane, index):
    half = nplane // 2
    return lax.select(index < half, 2 * index, 2 * (nplane - 1 - index) + 1)


def ring_index(nplane, plane):
    row = lax.div(plane, 2)
    return lax.select(lax.rem(plane, 2) == 0, row, nplane - 1 - row)


def offsets(nep):
    return [0] + [side * back for back in range(1, nep) for side in (-1, 1)]


def gather_order(parts, nplane, nep):
    far = nplane // 2
    events = []
    for off in offsets(nep):
        at = LINE_STEP * abs(off)
        if off:
            events.append((at, 1, ("note line", 0, 0, off, 0)))
        for d in range(1, far + 1):
            events.append((at + RING_STEP * d, 1 + d, ("note ring", 0, 0, off, d)))
    events.append((LINE_STEP * (nep - 1) + RING_STEP * far, 2 + far, ("tables", 0, 0, 0, 0)))
    for index, (kind, _, _, start) in enumerate(parts):
        events.append((start, 0, ("own", index, 0, 0, 0)))
        last = start
        if kind == "line":
            for off in offsets(nep):
                at = start + LINE_STEP * abs(off)
                if off:
                    events.append((at, 1, ("line", index, 0, off, 0)))
                for d in range(1, far + 1):
                    last = max(last, at + RING_STEP * d)
                    events.append((at + RING_STEP * d, 1 + d, ("ring", index, 0, off, d)))
        else:
            for d in range(1, far + 1):
                events.append((start + RING_STEP * d, 1 + d, ("ring", index, 0, 0, d)))
            for q in range(nplane):
                for off in offsets(nep)[1:]:
                    at = start + RING_STEP * min(q, nplane - q) + DEEP_STEP * abs(off)
                    last = max(last, at)
                    events.append((at, 2 + far, ("line", index, q, off, 0)))
        events.append((last, 3 + far, ("pick", index, 0, 0, 0)))
        for piece in range(PIECES):
            events.append((last + PRODUCT_STEP * (piece + 1), 4 + far, ("product", index, piece, 0, 0)))
    events.sort()
    return [event for _, _, event in events]


def scatter_order(parts, nplane, nep):
    far = nplane // 2
    events = []
    for index, (kind, _, _, start) in enumerate(parts):
        events.append((start, 0, ("down", index, 0, 0, 0)))
        begin = start + SPREAD_STEP
        events.append((begin, 1, ("spread", index, 0, 0, 0)))
        if kind == "line":
            for off in offsets(nep):
                for d in range(far, -1, -1):
                    at = begin + BACK_RING * (far - d)
                    if d == 0:
                        at = at + BACK_LINE * (nep - 1 - abs(off))
                    events.append((at, 2 + nep - abs(off), ("ring", index, 0, off, d)))
        else:
            for q in range(nplane):
                for off in offsets(nep):
                    at = begin + BACK_DEEP * (nep - 1 - abs(off))
                    events.append((at, 2 + nep - abs(off), ("line", index, q, off, 0)))
            done = begin + BACK_DEEP * (nep - 1)
            for d in range(far, -1, -1):
                events.append((done + BACK_RING * (far - d), 3 + nep, ("ring", index, 0, 0, d)))
    events.sort(key=lambda event: (event[0], event[1], event[2][1], event[2][2], -event[2][3], -event[2][4]))
    return [event for _, _, event in events]


def layer_kernel(
    plan, hot_ref, tok_ref, ids_ref, picks_ref, gates_ref, wg_hbm, wu_hbm, wd_hbm, out_ref, load_ref,
    xs, notes, route, sel, back, wg, wu, wd, inputs, stage, acc_g, acc_u, hidden, pairs, stage2, parts_ref,
    ring_land, line_land, count_own, count_in,
    own_sem, w_sem, note_recv, note_send, x_recv, x_send, swap_send, swap_recv, ring_recv, line_recv, out_send,
):
    nplane, nep, most, into, outof = plan
    far = nplane // 2
    count = nplane * nep
    rows, width = out_ref.shape
    top = ids_ref.shape[0]
    total = count * rows
    cap = stage.shape[0]
    ngroup = 2 * nplane
    group = lax.axis_index("group")
    ep = lax.axis_index("ep")
    core = lax.rem(group, 2)
    me_ring = ring_index(nplane, lax.div(group, 2))
    partner_group = group + 1 - 2 * core
    partner = (partner_group, ep)
    f32 = jnp.float32
    bf16 = jnp.bfloat16

    def spot(q):
        return lax.rem(me_ring + q + nplane, nplane)

    def ring_peer(side):
        return (ring_spot(nplane, spot(side)) * 2 + core, ep)

    peers = {1: ring_peer(1), -1: ring_peer(-1)}
    line_peers = {1: (group, lax.min(ep + 1, nep - 1)), -1: (group, lax.max(ep - 1, 0))}
    has = {1: ep < nep - 1, -1: ep > 0}

    def valid(off):
        if off == 0:
            return None
        return (ep + off < nep) if off > 0 else (ep + off >= 0)

    def both(a, b):
        if a is None:
            return b
        return a if b is None else a & b

    def when(cond, run):
        if cond is None:
            run()
        else:
            pl.when(cond)(run)

    waits = []

    def copy(src, dst, send, recv, target):
        return pltpu.make_async_remote_copy(
            src_ref=src, dst_ref=dst, send_sem=send, recv_sem=recv, device_id=target, device_id_type=MESH
        )

    def launch(cond, make):
        when(cond, lambda: make().start())
        waits.append((cond, make))

    own_block = me_ring * nep + ep
    own_copies = []
    for index, (_, c0, cols, _) in enumerate(into):
        made = pltpu.make_async_copy(
            tok_ref.at[:, pl.ds(c0, cols)], xs.at[own_block, :, pl.ds(c0, cols)], own_sem.at[index]
        )
        made.start()
        own_copies.append(made)
    weight_copies = []
    for index, (src, dst) in enumerate(((wg_hbm, wg), (wu_hbm, wu), (wd_hbm, wd))):
        made = pltpu.make_async_copy(src, dst, w_sem.at[index])
        made.start()
        weight_copies.append(made)

    barrier = pltpu.get_barrier_semaphore()
    for target in (partner, peers[1], peers[-1]):
        pl.semaphore_signal(barrier, inc=1, device_id=target, device_id_type=MESH)
    for side in (1, -1):
        @pl.when(has[side])
        def _(side=side):
            pl.semaphore_signal(barrier, inc=1, device_id=line_peers[side], device_id_type=MESH)

    note = notes.at[own_block]
    note[...] = jnp.zeros(note.shape, f32)
    note[:, pl.ds(0, rows)] = ids_ref[...].astype(f32)
    note[:, pl.ds(rows, rows)] = picks_ref[...].astype(f32)
    note[:, pl.ds(2 * rows, rows)] = gates_ref[...]
    pl.semaphore_wait(barrier, 3 + has[1].astype(jnp.int32) + has[-1].astype(jnp.int32))

    used = {"note": 0, "x": 0, "out": 0}

    def place(index, half, block):
        return x_recv.at[index, half, block]

    def x_copy(index, half, block, cols, send, target):
        part = xs.at[block, :, pl.ds(cols[0], cols[1])]
        return copy(part, part, x_send.at[send], place(index, half, block), target)

    def x_launch(cond, index, half, block, cols, target):
        send = used["x"]
        used["x"] += 1
        launch(cond, lambda: x_copy(index, half, block, cols, send, target))

    def x_wait(index, half, block, cols):
        x_copy(index, half, block, cols, 0, partner).wait_recv()

    def halves(c0, cols):
        return {1: (0, (c0, cols // 2)), -1: (1, (c0 + cols // 2, cols // 2))}

    def ring_out(cond, index, block, side, d):
        _, c0, cols, _ = into[index]
        half, span = (0, (c0, cols)) if d < far else halves(c0, cols)[side]
        x_launch(cond, index, half, block, span, peers[side])

    def line_out(index, q, off, side):
        _, c0, cols, _ = into[index]
        cond = both(valid(off), has[side])
        x_launch(cond, index, 0, spot(q) * nep + ep + off, (c0, cols), line_peers[side])

    def note_launch(cond, block, target):
        send = used["note"]
        used["note"] += 1
        launch(cond, lambda: copy(
            notes.at[block], notes.at[block], note_send.at[send], note_recv.at[block], target))

    def note_wait(block):
        copy(notes.at[block], notes.at[block], note_send.at[0], note_recv.at[block], partner).wait_recv()

    def note_own():
        for side in (1, -1):
            note_launch(has[side], own_block, line_peers[side])
        for side in (1, -1):
            if far > 1 or side > 0:
                note_launch(None, own_block, peers[side])

    def note_line(off):
        block = me_ring * nep + ep + off
        when(valid(off), lambda: note_wait(block))
        side = 1 if off < 0 else -1
        note_launch(both(valid(off), has[side]), block, line_peers[side])
        for way in (1, -1):
            if far > 1 or way > 0:
                note_launch(valid(off), block, peers[way])

    def note_ring(off, d):
        for side in (1, -1):
            if d == far and side < 0:
                continue
            block = spot(-side * d) * nep + ep + off
            when(valid(off), lambda: note_wait(block))
            if d < far and (d + 1 < far or side > 0):
                note_launch(valid(off), block, peers[side])

    def gather_own(index):
        own_copies[index].wait()
        for side in (1, -1):
            line_out(index, 0, 0, side)
        for side in (1, -1):
            ring_out(None, index, own_block, side, 1)

    def gather_line(index, q, off):
        kind, c0, cols, _ = into[index]
        block = spot(q) * nep + ep + off
        when(valid(off), lambda: x_wait(index, 0, block, (c0, cols)))
        line_out(index, q, off, 1 if off < 0 else -1)
        if kind == "line":
            for side in (1, -1):
                ring_out(valid(off), index, block, side, 1)

    def gather_ring(index, off, d):
        kind, c0, cols, _ = into[index]
        for side in (1, -1):
            block = spot(-side * d) * nep + ep + off
            half, span = (0, (c0, cols)) if d < far else halves(c0, cols)[side]
            when(valid(off), lambda: x_wait(index, half, block, span))
            if d < far:
                ring_out(valid(off), index, block, side, d + 1)
                if kind == "ring":
                    for way in (1, -1):
                        line_out(index, -side * d, 0, way)
        if d == far and kind == "ring":
            for way in (1, -1):
                line_out(index, far, 0, way)

    def tables():
        lane = lax.broadcasted_iota(jnp.int32, (top, 128), 1)
        fit = 128 // rows
        for chunk in range(total // 128):
            for what in range(3):
                piece = jnp.zeros((top, 128), f32)
                for j in range(fit):
                    tile = notes[chunk * fit + j]
                    turn = (rows * (j - what)) % 128
                    if turn:
                        tile = pltpu.roll(tile, turn, 1)
                    piece = jnp.where(lax.div(lane, rows) == j, tile, piece)
                route[what, :, pl.ds(chunk * 128, 128)] = piece
        expert = group * nep + ep
        other = partner_group * nep + ep
        hot = (hot_ref[ep] * nep + ep).astype(f32)
        expert_f, other_f = expert.astype(f32), other.astype(f32)
        block_rows = rows // 2
        a = lax.broadcasted_iota(jnp.int32, (128, 128), 0)
        b = lax.broadcasted_iota(jnp.int32, (128, 128), 1)
        before = ((lax.div(a, block_rows) == lax.div(b, block_rows)) & (a < b)).astype(f32)
        sub = lax.broadcasted_iota(jnp.int32, (8, 128), 0)
        lane8 = lax.broadcasted_iota(jnp.int32, (8, 128), 1)
        slot = lax.broadcasted_iota(jnp.int32, (cap, 128), 0).astype(f32)
        sums = [jnp.zeros((1, 1), f32) for _ in range(4)]

        def add_up(flag):
            return jnp.sum(jnp.sum(flag.astype(f32), axis=1, keepdims=True), axis=0, keepdims=True)

        for chunk in range(total // 128):
            at = pl.ds(chunk * 128, 128)
            ids, picks, gates = route[0, :, at], route[1, :, at], route[2, :, at]
            chosen = [ids == expert_f, ids == other_f]
            flag = [jnp.sum(c.astype(f32), axis=0, keepdims=True) for c in chosen]
            scale = [jnp.sum(jnp.where(c, gates, 0.0), axis=0, keepdims=True) for c in chosen]
            stacked = jnp.where(sub == 0, flag[0], jnp.where(sub == 1, flag[1], 0.0))
            rank = jnp.dot(stacked, before, preferred_element_type=f32)
            first = (lax.div(lane8[0:1], block_rows) + chunk * (128 // block_rows)).astype(f32) * most
            scaled = []
            for which in range(2):
                position = jnp.where(flag[which] > 0, first + rank[which:which + 1], -1.0)
                one = (slot == position).astype(f32)
                sel[pl.ds(which * cap, cap), at] = one.astype(bf16)
                scaled.append(one * scale[which])
            back[at, :] = jnp.concatenate(scaled, axis=0).T.astype(bf16)
            copied = (ids == hot) & (picks < ngroup)
            for which, (here, its) in enumerate(((expert_f, group), (other_f, partner_group))):
                sums[2 * which] = sums[2 * which] + add_up((ids == here) & ~copied)
                sums[2 * which + 1] = sums[2 * which + 1] + add_up(copied & (picks == its.astype(f32)))
        lane_n = lane8
        count_own[0] = jnp.where(lane_n == 0, sums[0], jnp.where(lane_n == 1, sums[1], 0.0))
        count_own[1] = jnp.where(lane_n == 0, sums[2], jnp.where(lane_n == 1, sums[3], 0.0))
        launch(None, count_copy)

    def count_copy():
        spare = len(into) + len(outof)
        return copy(count_own.at[1], count_in, swap_send.at[spare], swap_recv.at[spare], partner)

    step = 256

    def in_copy(index):
        _, c0, cols, _ = into[index]
        return copy(
            stage.at[:, pl.ds(c0, cols)], inputs.at[pl.ds(cap, cap), pl.ds(c0, cols)],
            swap_send.at[index], swap_recv.at[index], partner,
        )

    def pick(index):
        _, c0, cols, _ = into[index]

        def part(i, _):
            at = pl.ds(pl.multiple_of(c0 + i * step, step), step)
            got = jnp.dot(sel[...], xs[:, :, at].reshape(total, step), preferred_element_type=f32).astype(bf16)
            inputs[pl.ds(0, cap), at] = got[:cap]
            stage[:, at] = got[cap:]
            return 0

        lax.fori_loop(0, cols // step, part, 0)
        launch(None, lambda: in_copy(index))

    seen = []

    def product(index, piece):
        _, c0, cols, _ = into[index]
        if piece == 0:
            in_copy(index).wait_recv()
            if not seen:
                weight_copies[0].wait()
                weight_copies[1].wait()
        first = piece not in seen
        seen.append(piece)
        tiles = acc_g.shape[1] // step // PIECES

        def part(j, _):
            at = pl.ds(pl.multiple_of((piece * tiles + j) * step, step), step)
            for weight, acc in ((wg, acc_g), (wu, acc_u)):
                got = jnp.dot(
                    inputs[:, pl.ds(c0, cols)], weight[pl.ds(c0, cols), at], preferred_element_type=f32
                )
                acc[:, at] = got if first else acc[:, at] + got
            return 0

        lax.fori_loop(0, tiles, part, 0)

    def activate():
        def part(i, _):
            at = pl.ds(pl.multiple_of(i * 32, 32), 32)
            gate = acc_g[at, :]
            hidden[at, :] = (gate / (1.0 + jnp.exp(-gate)) * acc_u[at, :]).astype(bf16)
            return 0

        lax.fori_loop(0, 2 * cap // 32, part, 0)

    def back_copy(index):
        _, c0, cols, _ = outof[index]
        spot_of = len(into) + index
        return copy(
            stage2.at[:, pl.ds(c0, cols)], pairs.at[pl.ds(cap, cap), pl.ds(c0, cols)],
            swap_send.at[spot_of], swap_recv.at[spot_of], partner,
        )

    def down(index):
        _, c0, cols, _ = outof[index]

        def part(i, _):
            at = pl.ds(pl.multiple_of(c0 + i * step, step), step)
            got = jnp.dot(hidden[...], wd[:, at], preferred_element_type=f32).astype(bf16)
            pairs[pl.ds(0, cap), at] = got[:cap]
            stage2[:, at] = got[cap:]
            return 0

        lax.fori_loop(0, cols // step, part, 0)
        launch(None, lambda: back_copy(index))

    def spread(index):
        _, c0, cols, _ = outof[index]
        back_copy(index).wait_recv()

        def part(i, _):
            at = pl.ds(pl.multiple_of(c0 + i * step, step), step)
            got = jnp.dot(back[...], pairs[:, at], preferred_element_type=f32).astype(bf16)
            parts_ref[:, :, at] = got.reshape(count, rows, step)
            return 0

        lax.fori_loop(0, cols // step, part, 0)

    def add(dst, sources):
        def part(i, _):
            at = pl.ds(pl.multiple_of(i * 16, 16), 16)
            value = sources[0][at, :].astype(f32)
            for source in sources[1:]:
                value = value + source[at, :].astype(f32)
            dst[at, :] = value.astype(dst.dtype)
            return 0

        lax.fori_loop(0, rows // 16, part, 0)

    def out_launch(cond, src, dst, recv, target):
        send = used["out"]
        used["out"] += 1
        launch(cond, lambda: copy(src, dst, out_send.at[send], recv, target))

    def way(side):
        return 0 if side > 0 else 1

    def ring_slot(index, side, d, half, e, span):
        c0, cols = span
        return (
            ring_land.at[way(side), d, e, :, pl.ds(c0, cols)],
            ring_recv.at[index, way(side), d, half, e],
        )

    def ring_send(cond, index, off, side, d, half, span):
        dst, recv = ring_slot(index, side, d - 1, half, ep + off, span)
        src = parts_ref.at[spot(side * d) * nep + ep + off, :, pl.ds(span[0], span[1])]
        out_launch(cond, src, dst, recv, peers[side])

    def ring_await(index, off, side, d, half, span):
        dst, recv = ring_slot(index, side, d, half, ep + off, span)
        copy(dst, dst, out_send.at[0], recv, partner).wait_recv()
        return dst

    def line_slot(index, side, q, e, span):
        c0, cols = span
        return (
            line_land.at[way(side), spot(q) * nep + e, :, pl.ds(c0, cols)],
            line_recv.at[index, way(side), spot(q) * nep + e],
        )

    def line_send(cond, index, q, off, side):
        _, c0, cols, _ = outof[index]
        dst, recv = line_slot(index, side, q, ep + off, (c0, cols))
        src = parts_ref.at[spot(q) * nep + ep + off, :, pl.ds(c0, cols)]
        out_launch(cond, src, dst, recv, line_peers[side])

    def line_await(index, side, q, off):
        _, c0, cols, _ = outof[index]
        dst, recv = line_slot(index, side, q, ep + off, (c0, cols))
        copy(dst, dst, out_send.at[0], recv, partner).wait_recv()
        return dst

    def block(q, off, span):
        return parts_ref.at[spot(q) * nep + ep + off, :, pl.ds(span[0], span[1])]

    def line_merge(index, q, off, sources, dst):
        left, right = has[-1], has[1]
        if off != 0:
            side = 1 if off > 0 else -1
            behind = has[-side]

            def go():
                @pl.when(behind)
                def _():
                    add(dst, sources + [line_await(index, side, q, off)])

                if len(sources) > 1:
                    @pl.when(jnp.logical_not(behind))
                    def _():
                        add(dst, sources)

            when(valid(off), go)
            line_send(valid(off), index, q, off, side)
        else:
            @pl.when(left & right)
            def _():
                add(dst, sources + [line_await(index, 1, q, 0), line_await(index, -1, q, 0)])

            @pl.when(left & jnp.logical_not(right))
            def _():
                add(dst, sources + [line_await(index, 1, q, 0)])

            @pl.when(right & jnp.logical_not(left))
            def _():
                add(dst, sources + [line_await(index, -1, q, 0)])

    def scatter_ring(index, off, d):
        kind, c0, cols, _ = outof[index]
        whole = (c0, cols)
        split = halves(c0, cols)
        if d == far:
            for side in (1, -1):
                half, span = split[side]
                ring_send(valid(off), index, off, side, d, half, span)
            if far > 1:
                for side in (1, -1):
                    half, span = split[-side]
                    ring_send(valid(off), index, off, side, d - 1, half, span)
        elif d > 0:
            for side in (1, -1):
                pieces = [split[side]] if d + 1 == far else [split[1], split[-1]]
                for half, span in pieces:
                    def go(half=half, span=span, side=side):
                        got = ring_await(index, off, side, d, half, span)
                        add(block(side * d, off, span), [block(side * d, off, span), got])

                    when(valid(off), go)
                    ring_send(valid(off), index, off, side, d, half, span)
        else:
            def take():
                pieces = {}
                for side in (1, -1):
                    for half, span in ([split[side]] if far == 1 else [split[1], split[-1]]):
                        ring_await(index, off, side, 0, half, span)

            when(valid(off), take)
            sources = [block(0, off, whole)]
            for side in (1, -1):
                sources.append(ring_slot(index, side, 0, 0, ep + off, whole)[0])
            if off != 0:
                line_merge(index, 0, off, sources, block(0, off, whole))
            elif kind == "line":
                line_merge(index, 0, 0, sources, out_ref.at[:, pl.ds(c0, cols)])
            else:
                add(out_ref.at[:, pl.ds(c0, cols)], sources)

    def scatter_line(index, q, off):
        _, c0, cols, _ = outof[index]
        line_merge(index, q, off, [block(q, off, (c0, cols))], block(q, off, (c0, cols)))

    note_own()
    for what, index, q, off, d in gather_order(into, nplane, nep):
        if what == "note line":
            note_line(off)
        elif what == "note ring":
            note_ring(off, d)
        elif what == "tables":
            tables()
        elif what == "own":
            gather_own(index)
        elif what == "line":
            gather_line(index, q, off)
        elif what == "ring":
            gather_ring(index, off, d)
        elif what == "pick":
            pick(index)
        else:
            product(index, q)
    activate()
    weight_copies[2].wait()
    for what, index, q, off, d in scatter_order(outof, nplane, nep):
        if what == "down":
            down(index)
        elif what == "spread":
            spread(index)
        elif what == "ring":
            scatter_ring(index, off, d)
        else:
            scatter_line(index, q, off)
    count_copy().wait_recv()
    load_ref[...] = (count_own[0] + count_in[...])[0:1, 0:2] / top
    for cond, make in waits:
        when(cond, lambda: make().wait_send())

def copies_of(parts, nplane, nep):
    far = nplane // 2
    spots = 2 * nep - 1
    notes = 2 + min(far, 2) + (spots - 1) * (1 + min(far, 2)) + spots * max(2 * far - 3, 0)
    sent, returned = 0, 0
    for kind, _, _, _ in parts:
        ring = 2 + 2 * min(far - 1, 1) + sum(2 if d + 1 == far else 4 for d in range(1, far))
        if kind == "line":
            sent += 4 + 3 * (spots - 1) + 2 * spots * (far - 1)
            returned += spots * ring + spots - 1
        else:
            sent += 4 + 6 * (far - 1) + 2 + nplane * (spots - 1)
            returned += nplane * (spots - 1) + ring
    return notes, sent, returned


def layer(tokens, ids, picks, gates, hot, w_gate, w_up, w_down, plan, shapes):
    nplane, nep, _, into, outof = plan
    far = nplane // 2
    count = nplane * nep
    rows, width = tokens.shape
    dma = pltpu.SemaphoreType.DMA
    vmem = pl.BlockSpec(memory_space=pltpu.VMEM)
    hbm = pl.BlockSpec(memory_space=pl.ANY)
    notes, sent, _ = copies_of(into, nplane, nep)
    returned = copies_of(outof, nplane, nep)[2]
    swaps = len(into) + len(outof) + 1
    return pl.pallas_call(
        functools.partial(layer_kernel, plan),
        out_shape=[
            jax.ShapeDtypeStruct((rows, width), tokens.dtype),
            jax.ShapeDtypeStruct((1, 2), jnp.float32),
        ],
        in_specs=[pl.BlockSpec(memory_space=pltpu.SMEM), hbm, vmem, vmem, vmem, hbm, hbm, hbm],
        out_specs=[vmem, vmem],
        scratch_shapes=[pltpu.VMEM(shape, kind) for shape, kind in shapes] + [
            dma((len(into),)), dma((3,)), dma((count,)), dma((notes,)),
            dma((len(into), 2, count)), dma((sent,)), dma((swaps,)), dma((swaps,)),
            dma((len(outof), 2, far, 2, nep)), dma((len(outof), 2, count)), dma((returned,)),
        ],
        compiler_params=pltpu.CompilerParams(
            collective_id=2, has_side_effects=True, vmem_limit_bytes=VMEM_LIMIT
        ),
    )(hot, tokens, ids, picks, gates, w_gate, w_up, w_down)


def buffers(nplane, nep, rows, width, top, hidden, cap, kind):
    count = nplane * nep
    total = count * rows
    f32 = jnp.float32
    return [
        ((count, rows, width), kind), ((count, top, 128), f32), ((3, top, total), f32),
        ((2 * cap, total), kind), ((total, 2 * cap), kind),
        ((width, hidden), kind), ((width, hidden), kind), ((hidden, width), kind),
        ((2 * cap, width), kind), ((cap, width), kind),
        ((2 * cap, hidden), f32), ((2 * cap, hidden), f32), ((2 * cap, hidden), kind),
        ((2 * cap, width), kind), ((cap, width), kind), ((count, rows, width), kind),
        ((2, nplane // 2, nep, rows, width), kind), ((2, count, rows, width), kind),
        ((2, 8, 128), f32), ((8, 128), f32),
    ]


def cuts(width, shares):
    unit = 256
    units = width // unit
    total = sum(share for _, share, _ in shares)
    made, at, seen = [], 0, 0
    for kind, share, start in shares:
        seen += share
        end = units * seen // total
        made.append((kind, at * unit, (end - at) * unit, start))
        at = end
    return tuple(made)


def body(
    tokens, expert_ids, gate_scores, replica_pick, replica_hot, gate_weight, up_weight, down_weight
):
    ngroup = lax.axis_size("group")
    nep = lax.axis_size("ep")
    nplane = ngroup // 2
    device_count = ngroup * nep
    group_index = lax.axis_index("group")
    ep_index = lax.axis_index("ep")
    core = group_index % 2
    me = group_index * nep + ep_index
    partner = (group_index + 1 - 2 * core) * nep + ep_index
    tok_dev, width = tokens.shape
    top_count = expert_ids.shape[1]
    most = (tok_dev // 2 * top_count + device_count - 1) // device_count + 1
    capacity = 2 * most * nplane * nep
    cut = width // 256 * 128
    back_cut = width * 11 // 14 // 128 * 128

    hidden = gate_weight.shape[2]
    plan_shapes = buffers(nplane, nep, tok_dev, width, top_count, hidden, capacity, tokens.dtype)
    need = sum(math.prod(shape) * jnp.dtype(kind).itemsize for shape, kind in plan_shapes)
    if nplane % 2 == 0 and need < VMEM_LIMIT * 7 // 8:
        plan = (nplane, nep, most, cuts(width, INTO), cuts(width, OUTOF))
        return layer(
            tokens, expert_ids.T, replica_pick.T, gate_scores.T, replica_hot,
            gate_weight[0], up_weight[0], down_weight[0], plan, plan_shapes,
        )

    coded = expert_ids * (ngroup + 1) + replica_pick
    note = jnp.concatenate([coded.astype(jnp.float32), gate_scores], axis=1).reshape(-1, 128)
    every, notes = gather_plane(tokens, note, nplane, nep, cut)
    every = every.reshape(nplane * nep * tok_dev, width)
    routing = notes.reshape(device_count * tok_dev, 2 * top_count)
    coded = routing[:, :top_count].astype(jnp.int32)
    ids = coded // (ngroup + 1)
    picks = coded % (ngroup + 1)
    hot = replica_hot[ep_index]
    replicated = (ids % nep == ep_index) & (ids // nep == hot) & (picks < ngroup)
    primary_load = jnp.sum(((ids == me) & ~replicated).astype(jnp.float32))
    replica_load = jnp.sum((replicated & (picks == group_index)).astype(jnp.float32))
    loads = jnp.stack([primary_load, replica_load])[None, :] / top_count

    mine = routing.reshape(nplane, 2, nep * tok_dev, 2 * top_count)
    mine = lax.dynamic_index_in_dim(mine, core, 1, keepdims=False).reshape(-1, 2 * top_count)
    my_ids = mine[:, :top_count].astype(jnp.int32) // (ngroup + 1)
    my_gates = mine[:, top_count:]

    def spots(expert):
        chosen = my_ids == expert
        mask = jnp.any(chosen, axis=1)
        scale = jnp.sum(jnp.where(chosen, my_gates, 0.0), axis=1)
        place = jnp.where(mask, jnp.cumsum(mask.astype(jnp.int32)) - 1, -1)
        spot = place[None, :] == jnp.arange(capacity, dtype=jnp.int32)[:, None]
        return spot, jnp.sum(jnp.where(spot, scale[None, :], 0.0), axis=1)

    spot_me, scale_me = spots(me)
    spot_other, scale_other = spots(partner)
    select = jnp.concatenate([spot_me, spot_other], axis=0).astype(jnp.bfloat16)
    row_scale = jnp.concatenate([scale_me, scale_other], axis=0)
    swap = [(index, index ^ 1) for index in range(ngroup)]

    picked = jnp.dot(select, every, preferred_element_type=jnp.float32).astype(jnp.bfloat16)
    inputs = jnp.concatenate(
        [picked[:capacity], lax.ppermute(picked[capacity:], "group", swap)], axis=0
    )
    gate_act = jnp.dot(inputs, gate_weight[0], preferred_element_type=jnp.float32)
    up_act = jnp.dot(inputs, up_weight[0], preferred_element_type=jnp.float32)
    hidden = (jax.nn.silu(gate_act) * up_act).astype(jnp.bfloat16)
    pair_out = jnp.dot(hidden, down_weight[0], preferred_element_type=jnp.float32).astype(jnp.bfloat16)
    pairs = jnp.concatenate(
        [pair_out[:capacity], lax.ppermute(pair_out[capacity:], "group", swap)], axis=0
    )
    scaled = (pairs.astype(jnp.float32) * row_scale[:, None]).astype(jnp.bfloat16)
    spread = lax.dot_general(
        select, scaled, (((0,), (0,)), ((), ())), preferred_element_type=jnp.float32
    ).astype(jnp.bfloat16)
    mixed = scatter_plane(spread.reshape(nplane, nep, tok_dev, width), back_cut)
    return mixed, loads


def solution(mesh):
    rows = P(AXES, None)
    weights = P(AXES, None, None)
    return jax.shard_map(
        body,
        mesh=mesh,
        in_specs=(rows, rows, rows, rows, P(), weights, weights, weights),
        out_specs=(rows, rows),
        check_vma=False,
    )
```

```python
import functools
import math

import jax
import jax.numpy as jnp
from jax import lax
from jax.experimental import pallas as pl
from jax.experimental.pallas import tpu as pltpu
from jax.sharding import PartitionSpec as P

AXES = ("group", "ep")
MESH = pl.DeviceIdType.MESH

LINE_STEP, RING_STEP, DEEP_STEP, PRODUCT_STEP = 1.1, 3.1, 2.3, 2.6
SPREAD_STEP, BACK_RING, BACK_LINE, BACK_DEEP = 1.1, 2.0, 0.7, 3.0
BACK_LAST = 2.8
PIECES = 2
POOL = 12
INTO = (("line", 4, 0.0), ("line", 4, 0.0), ("line", 3, 5.0), ("ring", 3, 0.0))
OUTOF = (("ring", 3, 1.1), ("line", 4, 1.5), ("line", 4, 6.4), ("line", 3, 4.4))
VMEM_LIMIT = 67043328


def place_of(nplane, nep):
    group = lax.axis_index("group")
    ep = lax.axis_index("ep")
    core = lax.rem(group, 2)
    plane = lax.div(group, 2)

    def plane_peer(step):
        other = lax.rem(plane + step, nplane)
        return other, (other * 2 + core, ep)

    def ep_peer(step):
        other = lax.rem(ep + step, nep)
        return other, (group, other)

    return plane, ep, plane_peer, ep_peer


def greet(nplane, nep, plane_peer, ep_peer):
    barrier = pltpu.get_barrier_semaphore()
    for step in range(1, nplane):
        pl.semaphore_signal(barrier, inc=1, device_id=plane_peer(step)[1], device_id_type=MESH)
    for step in range(1, nep):
        pl.semaphore_signal(barrier, inc=1, device_id=ep_peer(step)[1], device_id_type=MESH)
    pl.semaphore_wait(barrier, nplane + nep - 2)


def gather_kernel(
    nplane, nep, cut, x_ref, note_ref, out_ref, notes_ref,
    own_sem, send_a, recv_a, send_b, recv_b, right_a, left_a, right_b, left_b, note_send, note_recv,
):
    plane, ep, plane_peer, ep_peer = place_of(nplane, nep)
    group = lax.axis_index("group")
    me = group * nep + ep
    total = 2 * nplane * nep
    width = x_ref.shape[1]
    cols = {"a": pl.ds(0, cut), "b": pl.ds(cut, width - cut)}
    recv = {"a": recv_a, "b": recv_b}
    rights = {"a": right_a, "b": right_b}
    lefts = {"a": left_a, "b": left_b}
    own = pltpu.make_async_copy(x_ref, out_ref.at[plane, ep], own_sem.at[0])
    own.start()
    own_note = pltpu.make_async_copy(note_ref, notes_ref.at[me], own_sem.at[1])
    own_note.start()

    barrier = pltpu.get_barrier_semaphore()
    for step in range(1, total):
        other = lax.rem(me + step, total)
        pl.semaphore_signal(
            barrier, inc=1, device_id=(lax.div(other, nep), lax.rem(other, nep)), device_id_type=MESH
        )
    pl.semaphore_wait(barrier, total - 1)

    def copy(src, p, e, half, send, target):
        return pltpu.make_async_remote_copy(
            src_ref=src.at[:, cols[half]],
            dst_ref=out_ref.at[p, e, :, cols[half]],
            send_sem=send,
            recv_sem=recv[half].at[p * nep + e],
            device_id=target,
            device_id_type=MESH,
        )

    sends = []
    used = {"a": 0, "b": 0}

    def push(src, p, e, half):
        send = send_a if half == "a" else send_b
        for step in range(1, nplane):
            made = copy(src, p, e, half, send.at[used[half]], plane_peer(step)[1])
            used[half] += 1
            made.start()
            sends.append(made)

    def arrived(p, e, half):
        copy(out_ref.at[p, e], p, e, half, send_a.at[0], ep_peer(1)[1]).wait_recv()

    def to_right(src, p, e, half):
        return copy(src, p, e, half, rights[half].at[p * nep + e], (group, lax.rem(ep + 1, nep)))

    def to_left(src, p, e, half):
        return copy(src, p, e, half, lefts[half].at[p * nep + e], (group, lax.rem(ep + nep - 1, nep)))

    has_right, has_left = ep < nep - 1, ep > 0

    def both_ways(src, p, half):
        @pl.when(has_right)
        def _():
            to_right(src, p, ep, half).start()

        @pl.when(has_left)
        def _():
            to_left(src, p, ep, half).start()

    def chain(p, back, half):
        @pl.when(ep - back >= 0)
        def _():
            arrived(p, ep - back, half)

            @pl.when(has_right)
            def _():
                to_right(out_ref.at[p, ep - back], p, ep - back, half).start()

        @pl.when(ep + back < nep)
        def _():
            arrived(p, ep + back, half)

            @pl.when(has_left)
            def _():
                to_left(out_ref.at[p, ep + back], p, ep + back, half).start()

    def chain_end(p, back, half):
        @pl.when((ep - back >= 0) & has_right)
        def _():
            to_right(out_ref.at[p, ep - back], p, ep - back, half).wait_send()

        @pl.when((ep + back < nep) & has_left)
        def _():
            to_left(out_ref.at[p, ep + back], p, ep + back, half).wait_send()

    def note(source, step, target):
        return pltpu.make_async_remote_copy(
            src_ref=note_ref,
            dst_ref=notes_ref.at[source],
            send_sem=note_send.at[step],
            recv_sem=note_recv.at[source],
            device_id=(lax.div(target, nep), lax.rem(target, nep)),
            device_id_type=MESH,
        )

    both_ways(x_ref, plane, "a")
    push(x_ref, plane, ep, "b")
    push(x_ref, plane, ep, "a")
    both_ways(x_ref, plane, "b")
    for step in range(1, total):
        note(me, step, lax.rem(me + step, total)).start()
    for back in range(1, max(nplane, nep)):
        if back < nep:
            chain(plane, back, "a")
        if back < nplane:
            source = lax.rem(plane + nplane - back, nplane)
            arrived(source, ep, "b")
            both_ways(out_ref.at[source, ep], source, "b")
        if back < nep:
            left_in, right_in = ep - back >= 0, ep + back < nep

            @pl.when(left_in)
            def _():
                for step in range(1, nplane):
                    copy(
                        out_ref.at[plane, ep - back], plane, ep - back, "a",
                        send_a.at[(nplane - 1) * back + step - 1], plane_peer(step)[1],
                    ).start()

            @pl.when(right_in)
            def _():
                for step in range(1, nplane):
                    copy(
                        out_ref.at[plane, ep + back], plane, ep + back, "a",
                        send_a.at[(nplane - 1) * (nep + back) + step - 1], plane_peer(step)[1],
                    ).start()
    for back in range(1, nep):
        for p_back in range(nplane):
            chain(lax.rem(plane + nplane - p_back, nplane), back, "b")
    for p_back in range(1, nplane):
        p = lax.rem(plane + nplane - p_back, nplane)
        for e in range(nep):
            arrived(p, e, "a")
    for step in range(1, total):
        source = lax.rem(me + total - step, total)
        note(source, step, lax.rem(me + 1, total)).wait_recv()
    for made in sends:
        made.wait_send()
    for back in range(1, nep):
        @pl.when(ep - back >= 0)
        def _():
            for step in range(1, nplane):
                copy(
                    out_ref.at[plane, ep - back], plane, ep - back, "a",
                    send_a.at[(nplane - 1) * back + step - 1], plane_peer(step)[1],
                ).wait_send()

        @pl.when(ep + back < nep)
        def _():
            for step in range(1, nplane):
                copy(
                    out_ref.at[plane, ep + back], plane, ep + back, "a",
                    send_a.at[(nplane - 1) * (nep + back) + step - 1], plane_peer(step)[1],
                ).wait_send()

    for back in range(nep):
        for half in ("a", "b"):
            for p_back in range(nplane if half == "b" else 1):
                p = lax.rem(plane + nplane - p_back, nplane)
                if back == 0:
                    @pl.when(has_right)
                    def _():
                        to_right(x_ref, p, ep, half).wait_send()

                    @pl.when(has_left)
                    def _():
                        to_left(x_ref, p, ep, half).wait_send()
                else:
                    chain_end(p, back, half)
    for step in range(1, total):
        note(me, step, lax.rem(me + step, total)).wait_send()
    own.wait()
    own_note.wait()


def gather_plane(tokens, note, nplane, nep, cut):
    rows, width = tokens.shape
    count = nplane * nep
    dma = pltpu.SemaphoreType.DMA
    vmem = pl.BlockSpec(memory_space=pltpu.VMEM)
    return pl.pallas_call(
        functools.partial(gather_kernel, nplane, nep, cut),
        out_shape=[
            jax.ShapeDtypeStruct((nplane, nep, rows, width), tokens.dtype),
            jax.ShapeDtypeStruct((2 * count,) + note.shape, note.dtype),
        ],
        in_specs=[vmem, vmem],
        out_specs=[vmem, vmem],
        scratch_shapes=[
            dma((2,)),
            dma((2 * (nplane - 1) * nep,)), dma((count,)), dma((nplane - 1,)), dma((count,)),
            dma((count,)), dma((count,)), dma((count,)), dma((count,)),
            dma((2 * count,)), dma((2 * count,)),
        ],
        compiler_params=pltpu.CompilerParams(collective_id=0, has_side_effects=True),
    )(tokens, note)


def scatter_kernel(
    nplane, nep, cut, part_ref, out_ref,
    land_a1, land_b1, mid_a, mid_b, land_a2, land_b2,
    send_a1, recv_a1, send_b1, recv_b1, send_a2, recv_a2, send_b2, recv_b2,
):
    plane, ep, plane_peer, ep_peer = place_of(nplane, nep)
    width = out_ref.shape[1]
    cols_a, cols_b = pl.ds(0, cut), pl.ds(cut, width - cut)
    greet(nplane, nep, plane_peer, ep_peer)

    def move(src, dst, send, recv, target):
        made = pltpu.make_async_remote_copy(
            src_ref=src, dst_ref=dst, send_sem=send, recv_sem=recv, device_id=target, device_id_type=MESH
        )
        made.start()
        return made

    first_a, first_b = {}, {}
    for item in range(1, max(nplane, nep) + 1):
        if item <= nep:
            e = lax.rem(ep + item, nep)
            for step in range(1, nplane):
                p, target = plane_peer(step)
                spot = (step - 1) * nep + item - 1
                first_a[item, step] = move(
                    part_ref.at[p, e, :, cols_a], land_a1.at[step - 1, item - 1],
                    send_a1.at[spot], recv_a1.at[spot], target,
                )
        if item <= nplane:
            p = lax.rem(plane + item, nplane)
            for step in range(1, nep):
                e, target = ep_peer(step)
                spot = (step - 1) * nplane + item - 1
                first_b[item, step] = move(
                    part_ref.at[p, e, :, cols_b], land_b1.at[step - 1, item - 1],
                    send_b1.at[spot], recv_b1.at[spot], target,
                )
    second_a, second_b = [], []
    for item in range(1, max(nplane, nep) + 1):
        if item <= nep:
            e, target = ep_peer(item)
            total = part_ref[plane, e, :, cols_a].astype(jnp.float32)
            for step in range(1, nplane):
                first_a[item, step].wait_recv()
                total = total + land_a1[step - 1, item - 1].astype(jnp.float32)
            if item < nep:
                mid_a[item - 1] = total.astype(mid_a.dtype)
                second_a.append(
                    move(mid_a.at[item - 1], land_a2.at[item - 1], send_a2.at[item - 1], recv_a2.at[item - 1], target)
                )
            else:
                total_a = total
        if item <= nplane:
            p, target = plane_peer(item)
            total = part_ref[p, ep, :, cols_b].astype(jnp.float32)
            for step in range(1, nep):
                first_b[item, step].wait_recv()
                total = total + land_b1[step - 1, item - 1].astype(jnp.float32)
            if item < nplane:
                mid_b[item - 1] = total.astype(mid_b.dtype)
                second_b.append(
                    move(mid_b.at[item - 1], land_b2.at[item - 1], send_b2.at[item - 1], recv_b2.at[item - 1], target)
                )
            else:
                total_b = total
    for index, made in enumerate(second_a):
        made.wait_recv()
        total_a = total_a + land_a2[index].astype(jnp.float32)
    out_ref[:, cols_a] = total_a.astype(out_ref.dtype)
    for index, made in enumerate(second_b):
        made.wait_recv()
        total_b = total_b + land_b2[index].astype(jnp.float32)
    out_ref[:, cols_b] = total_b.astype(out_ref.dtype)
    for made in list(first_a.values()) + list(first_b.values()) + second_a + second_b:
        made.wait_send()


def scatter_plane(parts, cut):
    nplane, nep, rows, width = parts.shape
    rest = width - cut
    kind = parts.dtype
    dma = pltpu.SemaphoreType.DMA
    pairs_a, pairs_b = (nplane - 1) * nep, (nep - 1) * nplane
    return pl.pallas_call(
        functools.partial(scatter_kernel, nplane, nep, cut),
        out_shape=jax.ShapeDtypeStruct((rows, width), kind),
        in_specs=[pl.BlockSpec(memory_space=pltpu.VMEM)],
        out_specs=pl.BlockSpec(memory_space=pltpu.VMEM),
        scratch_shapes=[
            pltpu.VMEM((nplane - 1, nep, rows, cut), kind),
            pltpu.VMEM((nep - 1, nplane, rows, rest), kind),
            pltpu.VMEM((nep - 1, rows, cut), kind),
            pltpu.VMEM((nplane - 1, rows, rest), kind),
            pltpu.VMEM((nep - 1, rows, cut), kind),
            pltpu.VMEM((nplane - 1, rows, rest), kind),
            dma((pairs_a,)), dma((pairs_a,)), dma((pairs_b,)), dma((pairs_b,)),
            dma((nep - 1,)), dma((nep - 1,)), dma((nplane - 1,)), dma((nplane - 1,)),
        ],
        compiler_params=pltpu.CompilerParams(collective_id=1, has_side_effects=True),
    )(parts)


def ring_spot(nplane, index):
    half = nplane // 2
    return lax.select(index < half, 2 * index, 2 * (nplane - 1 - index) + 1)


def ring_index(nplane, plane):
    row = lax.div(plane, 2)
    return lax.select(lax.rem(plane, 2) == 0, row, nplane - 1 - row)


def offsets(nep):
    return [0] + [side * back for back in range(1, nep) for side in (-1, 1)]


def gather_order(parts, nplane, nep):
    far = nplane // 2
    events = []
    for index, (kind, _, _, start) in enumerate(parts):
        events.append((start, 0, ("own", index, 0, 0, 0)))
        last = start
        if kind == "line":
            for off in offsets(nep):
                at = start + LINE_STEP * abs(off)
                if off:
                    events.append((at, 1, ("line", index, 0, off, 0)))
                for d in range(1, far + 1):
                    last = max(last, at + RING_STEP * d)
                    events.append((at + RING_STEP * d, 1 + d, ("ring", index, 0, off, d)))
        else:
            for d in range(1, far + 1):
                events.append((start + RING_STEP * d, 1 + d, ("ring", index, 0, 0, d)))
            for q in range(nplane):
                for off in offsets(nep)[1:]:
                    at = start + RING_STEP * min(q, nplane - q) + DEEP_STEP * abs(off)
                    last = max(last, at)
                    events.append((at, 2 + far, ("line", index, q, off, 0)))
        if index == 0:
            events.append((last, 3 + far, ("tables", index, 0, 0, 0)))
        events.append((last, 4 + far, ("pick", index, 0, 0, 0)))
        for piece in range(PIECES):
            events.append((last + PRODUCT_STEP * (piece + 1), 5 + far, ("product", index, piece, 0, 0)))
    events.sort()
    return [event for _, _, event in events]


def scatter_order(parts, nplane, nep):
    far = nplane // 2
    events = []
    for index, (kind, _, _, start) in enumerate(parts):
        events.append((start, 0, ("down", index, 0, 0, 0)))
        begin = start + SPREAD_STEP
        events.append((begin, 1, ("spread", index, 0, 0, 0)))
        if kind == "line":
            for off in offsets(nep):
                for d in range(far, -1, -1):
                    at = begin + BACK_RING * (far - d) + BACK_LINE * (nep - 1 - abs(off))
                    events.append((at, 2 + nep - abs(off), ("ring", index, 0, off, d)))
            at = begin + BACK_RING * far + BACK_LINE * (nep - 1) + BACK_LAST
            events.append((at, 3 + nep, ("last", index, 0, 0, 0)))
        else:
            for q in range(nplane):
                for off in offsets(nep):
                    at = begin + BACK_DEEP * (nep - 1 - abs(off))
                    events.append((at, 2 + nep - abs(off), ("line", index, q, off, 0)))
            done = begin + BACK_DEEP * (nep - 1)
            for d in range(far, -1, -1):
                events.append((done + BACK_RING * (far - d), 3 + nep, ("ring", index, 0, 0, d)))
    events.sort(key=lambda event: (event[0], event[1], event[2][1], event[2][2], -event[2][3], -event[2][4]))
    return [event for _, _, event in events]


def layer_kernel(
    plan, hot_ref, tok_ref, ids_ref, picks_ref, gates_ref, wg_hbm, wu_hbm, wd_hbm, out_ref, load_ref,
    xs, sel, back, wg, wu, wd, inputs, stage, acc_g, acc_u, hidden, pairs, stage2, parts_ref,
    ring_land, line_land, deep_land, count_own, count_in,
    own_sem, w_sem, pool_ring, pool_line, x_ring, x_line, swap_send, swap_recv, ring_recv, line_recv, deep_recv,
):
    nplane, nep, most, into, outof = plan
    far = nplane // 2
    count = nplane * nep
    rows, width = out_ref.shape
    top = ids_ref.shape[0]
    total = count * rows
    cap = stage.shape[0]
    ngroup = 2 * nplane
    group = lax.axis_index("group")
    ep = lax.axis_index("ep")
    core = lax.rem(group, 2)
    me_ring = ring_index(nplane, lax.div(group, 2))
    partner_group = group + 1 - 2 * core
    partner = (partner_group, ep)
    f32 = jnp.float32
    bf16 = jnp.bfloat16

    def spot(q):
        return lax.rem(me_ring + q + nplane, nplane)

    def ring_peer(side):
        return (ring_spot(nplane, spot(side)) * 2 + core, ep)

    peers = {1: ring_peer(1), -1: ring_peer(-1)}
    line_peers = {1: (group, lax.min(ep + 1, nep - 1)), -1: (group, lax.max(ep - 1, 0))}
    has = {1: ep < nep - 1, -1: ep > 0}

    def valid(off):
        if off == 0:
            return None
        return (ep + off < nep) if off > 0 else (ep + off >= 0)

    def both(a, b):
        if a is None:
            return b
        return a if b is None else a & b

    def when(cond, run):
        if cond is None:
            run()
        else:
            pl.when(cond)(run)

    pools = {key: [] for key in (("ring", 1), ("ring", -1), ("line", 1), ("line", -1))}
    swaps = []

    def copy(src, dst, send, recv, target):
        return pltpu.make_async_remote_copy(
            src_ref=src, dst_ref=dst, send_sem=send, recv_sem=recv, device_id=target, device_id_type=MESH
        )

    def send_out(cond, kind, side, make):
        pool = pools[kind, side]
        sems = (pool_ring if kind == "ring" else pool_line).at[0 if side > 0 else 1]
        turn = len(pool) % sems.shape[0]
        if len(pool) >= sems.shape[0]:
            old_cond, old = pool[-sems.shape[0]]
            when(old_cond, lambda: old().wait_send())

        def ready():
            return make(sems.at[turn])

        when(cond, lambda: ready().start())
        pool.append((cond, ready))

    def swap(make):
        make().start()
        swaps.append(make)

    lead = xs.shape[2] - width
    own_block = me_ring * nep + ep
    own_copies = []
    for index, (_, c0, cols, _) in enumerate(into):
        made = pltpu.make_async_copy(
            tok_ref.at[:, pl.ds(c0, cols)], xs.at[own_block, :, pl.ds(lead + c0, cols)], own_sem.at[index]
        )
        made.start()
        own_copies.append(made)
    weight_copies = []
    for index, (src, dst) in enumerate(((wg_hbm, wg), (wu_hbm, wu), (wd_hbm, wd))):
        made = pltpu.make_async_copy(src, dst, w_sem.at[index])
        made.start()
        weight_copies.append(made)

    barrier = pltpu.get_barrier_semaphore()
    for target in (partner, peers[1], peers[-1]):
        pl.semaphore_signal(barrier, inc=1, device_id=target, device_id_type=MESH)
    for side in (1, -1):
        @pl.when(has[side])
        def _(side=side):
            pl.semaphore_signal(barrier, inc=1, device_id=line_peers[side], device_id_type=MESH)

    own = jnp.concatenate(
        [ids_ref[...].astype(f32), picks_ref[...].astype(f32), gates_ref[...]], axis=0
    )
    own = jnp.concatenate([own, jnp.zeros((3 * top, lead - rows), f32)], axis=1)
    own = jnp.concatenate([own, jnp.zeros((lead - 3 * top, lead), f32)], axis=0)
    xs[own_block, :, pl.ds(0, lead)] = own.T[:rows].astype(bf16)
    pl.semaphore_wait(barrier, 3 + has[1].astype(jnp.int32) + has[-1].astype(jnp.int32))

    def span_of(index):
        _, c0, cols, _ = into[index]
        return (0, lead + cols) if c0 == 0 else (lead + c0, cols)

    def x_launch(cond, sem, kind, side, block, cols, target):
        part = xs.at[block, :, pl.ds(cols[0], cols[1])]
        send_out(cond, kind, side, lambda send: copy(part, part, send, sem, target))

    def x_wait(sem, blocks, cols):
        part = xs.at[pl.ds(0, blocks), :, pl.ds(cols[0], cols[1])]
        copy(part, part, pool_ring.at[0, 0], sem, partner).wait_recv()

    def halves(c0, cols):
        low = cols // 256 * 128
        return {1: (c0, low), -1: (c0 + low, cols - low)}

    starts_x = [0]
    for kind, _, _, _ in into:
        starts_x.append(starts_x[-1] + (nep if kind == "line" else count))

    def line_sem(index, q, off):
        at = starts_x[index] + ep + off
        return x_line.at[at if into[index][0] == "line" else at + spot(q) * nep]

    def ring_out(cond, index, block, off, side, d):
        span = span_of(index) if d < far else halves(*span_of(index))[side]
        x_launch(cond, x_ring.at[index, d - 1, ep + off], "ring", side, block, span, peers[side])

    def line_out(index, q, off, side):
        cond = both(valid(off), has[side])
        block = spot(q) * nep + ep + off
        x_launch(cond, line_sem(index, q, off), "line", side, block, span_of(index), line_peers[side])

    def gather_own(index):
        own_copies[index].wait()
        for side in (1, -1):
            line_out(index, 0, 0, side)
        for side in (1, -1):
            ring_out(None, index, own_block, 0, side, 1)

    def gather_line(index, q, off):
        block = spot(q) * nep + ep + off
        when(valid(off), lambda: x_wait(line_sem(index, q, off), 1, span_of(index)))
        line_out(index, q, off, 1 if off < 0 else -1)
        if into[index][0] == "line":
            for side in (1, -1):
                ring_out(valid(off), index, block, off, side, 1)

    def gather_ring(index, off, d):
        sem = x_ring.at[index, d - 1, ep + off]
        when(valid(off), lambda: x_wait(sem, 2 if d < far else 1, span_of(index)))
        for side in (1, -1):
            if d < far:
                block = spot(-side * d) * nep + ep + off
                ring_out(valid(off), index, block, off, side, d + 1)
                if into[index][0] == "ring":
                    for way in (1, -1):
                        line_out(index, -side * d, 0, way)
        if d == far and into[index][0] == "ring":
            for way in (1, -1):
                line_out(index, far, 0, way)

    def tables():
        expert = group * nep + ep
        other = partner_group * nep + ep
        hot = (hot_ref[ep] * nep + ep).astype(f32)
        expert_f, other_f = expert.astype(f32), other.astype(f32)
        block_rows = rows // 2
        a = lax.broadcasted_iota(jnp.int32, (128, 128), 0)
        b = lax.broadcasted_iota(jnp.int32, (128, 128), 1)
        before = ((lax.div(a, block_rows) == lax.div(b, block_rows)) & (a < b)).astype(f32)
        sub = lax.broadcasted_iota(jnp.int32, (8, 128), 0)
        lane8 = lax.broadcasted_iota(jnp.int32, (8, 128), 1)
        slot = lax.broadcasted_iota(jnp.int32, (cap, 128), 0).astype(f32)
        sums = [jnp.zeros((1, 1), f32) for _ in range(4)]

        def add_up(flag):
            return jnp.sum(jnp.sum(flag.astype(f32), axis=1, keepdims=True), axis=0, keepdims=True)

        for chunk in range(total // 128):
            at = pl.ds(chunk * 128, 128)
            fit = 128 // rows
            tile = xs[pl.ds(chunk * fit, fit), :, pl.ds(0, lead)].reshape(128, lead).astype(f32).T
            ids, picks, gates = tile[:top], tile[top:2 * top], tile[2 * top:3 * top]
            chosen = [ids == expert_f, ids == other_f]
            flag = [jnp.sum(c.astype(f32), axis=0, keepdims=True) for c in chosen]
            scale = [jnp.sum(jnp.where(c, gates, 0.0), axis=0, keepdims=True) for c in chosen]
            stacked = jnp.where(sub == 0, flag[0], jnp.where(sub == 1, flag[1], 0.0))
            rank = jnp.dot(stacked, before, preferred_element_type=f32)
            first = (lax.div(lane8[0:1], block_rows) + chunk * (128 // block_rows)).astype(f32) * most
            scaled = []
            for which in range(2):
                position = jnp.where(flag[which] > 0, first + rank[which:which + 1], -1.0)
                one = (slot == position).astype(f32)
                sel[pl.ds(which * cap, cap), at] = one.astype(bf16)
                scaled.append(one * scale[which])
            back[at, :] = jnp.concatenate(scaled, axis=0).T.astype(bf16)
            copied = (ids == hot) & (picks < ngroup)
            for which, (here, its) in enumerate(((expert_f, group), (other_f, partner_group))):
                sums[2 * which] = sums[2 * which] + add_up((ids == here) & ~copied)
                sums[2 * which + 1] = sums[2 * which + 1] + add_up(copied & (picks == its.astype(f32)))
        lane_n = lane8
        count_own[0] = jnp.where(lane_n == 0, sums[0], jnp.where(lane_n == 1, sums[1], 0.0))
        count_own[1] = jnp.where(lane_n == 0, sums[2], jnp.where(lane_n == 1, sums[3], 0.0))
        swap(count_copy)

    def count_copy():
        spare = len(into) + len(outof)
        return copy(count_own.at[1], count_in, swap_send.at[spare], swap_recv.at[spare], partner)

    step = 256

    def in_copy(index):
        _, c0, cols, _ = into[index]
        return copy(
            stage.at[:, pl.ds(c0, cols)], inputs.at[pl.ds(cap, cap), pl.ds(c0, cols)],
            swap_send.at[index], swap_recv.at[index], partner,
        )

    def pick(index):
        _, c0, cols, _ = into[index]

        def part(i, _):
            at = pl.ds(pl.multiple_of(c0 + i * step, step), step)
            here = pl.ds(pl.multiple_of(lead + c0 + i * step, 128), step)
            got = jnp.dot(sel[...], xs[:, :, here].reshape(total, step), preferred_element_type=f32).astype(bf16)
            inputs[pl.ds(0, cap), at] = got[:cap]
            stage[:, at] = got[cap:]
            return 0

        lax.fori_loop(0, cols // step, part, 0)
        swap(lambda: in_copy(index))

    seen = []

    def product(index, piece):
        _, c0, cols, _ = into[index]
        if piece == 0:
            in_copy(index).wait_recv()
            if not seen:
                weight_copies[0].wait()
                weight_copies[1].wait()
        first = piece not in seen
        seen.append(piece)
        tiles = acc_g.shape[1] // step // PIECES

        def part(j, _):
            at = pl.ds(pl.multiple_of((piece * tiles + j) * step, step), step)
            for weight, acc in ((wg, acc_g), (wu, acc_u)):
                got = jnp.dot(
                    inputs[:, pl.ds(c0, cols)], weight[pl.ds(c0, cols), at], preferred_element_type=f32
                )
                acc[:, at] = got if first else acc[:, at] + got
            return 0

        lax.fori_loop(0, tiles, part, 0)

    def activate():
        def part(i, _):
            at = pl.ds(pl.multiple_of(i * 32, 32), 32)
            gate = acc_g[at, :]
            hidden[at, :] = (gate / (1.0 + jnp.exp(-gate)) * acc_u[at, :]).astype(bf16)
            return 0

        lax.fori_loop(0, 2 * cap // 32, part, 0)

    def back_copy(index):
        _, c0, cols, _ = outof[index]
        spot_of = len(into) + index
        return copy(
            stage2.at[:, pl.ds(c0, cols)], pairs.at[pl.ds(cap, cap), pl.ds(c0, cols)],
            swap_send.at[spot_of], swap_recv.at[spot_of], partner,
        )

    def down(index):
        _, c0, cols, _ = outof[index]

        def part(i, _):
            at = pl.ds(pl.multiple_of(c0 + i * step, step), step)
            got = jnp.dot(hidden[...], wd[:, at], preferred_element_type=f32).astype(bf16)
            pairs[pl.ds(0, cap), at] = got[:cap]
            stage2[:, at] = got[cap:]
            return 0

        lax.fori_loop(0, cols // step, part, 0)
        swap(lambda: back_copy(index))

    def spread(index):
        _, c0, cols, _ = outof[index]
        back_copy(index).wait_recv()

        def part(i, _):
            at = pl.ds(pl.multiple_of(c0 + i * step, step), step)
            got = jnp.dot(back[...], pairs[:, at], preferred_element_type=f32).astype(bf16)
            parts_ref[:, :, at] = got.reshape(count, rows, step)
            return 0

        lax.fori_loop(0, cols // step, part, 0)

    def add(dst, sources):
        def part(i, _):
            at = pl.ds(pl.multiple_of(i * 16, 16), 16)
            value = sources[0][at, :].astype(f32)
            for source in sources[1:]:
                value = value + source[at, :].astype(f32)
            dst[at, :] = value.astype(dst.dtype)
            return 0

        lax.fori_loop(0, rows // 16, part, 0)

    def way(side):
        return 0 if side > 0 else 1

    starts_r = [0]
    for kind, _, _, _ in outof:
        starts_r.append(starts_r[-1] + (nep if kind == "line" else 1))

    def ring_sem(index, d, off):
        return ring_recv.at[starts_r[index] + (ep + off if outof[index][0] == "line" else 0), d]

    def ring_slot(side, d, off, span):
        return ring_land.at[way(side), d, ep + off, :, pl.ds(span[0], span[1])]

    def ring_send(cond, index, off, side, d, span):
        dst = ring_slot(side, d - 1, off, span)
        src = block(side * d, off, span)
        send_out(
            cond, "ring", side, lambda send: copy(src, dst, send, ring_sem(index, d - 1, off), peers[side])
        )

    def ring_await(index, off, d, blocks):
        _, c0, cols, _ = outof[index]
        part = ring_land.at[0, 0, pl.ds(0, blocks), :, pl.ds(c0, cols)]
        copy(part, part, pool_ring.at[0, 0], ring_sem(index, d, off), partner).wait_recv()

    def deep_slot(side, q, off, span):
        return deep_land.at[way(side), spot(q) * nep + ep + off, :, pl.ds(span[0], span[1])]

    def deep_sem(index, side, q, off):
        return deep_recv.at[deep_of[index], way(side), spot(q) * nep + ep + off]

    deep_of, lined = {}, {}
    for index, (kind, _, _, _) in enumerate(outof):
        if kind == "line":
            lined[index] = len(lined)
        else:
            deep_of[index] = len(deep_of)

    def deep_send(cond, index, q, off, side):
        _, c0, cols, _ = outof[index]
        src, dst = block(q, off, (c0, cols)), deep_slot(side, q, off, (c0, cols))
        send_out(
            cond, "line", side, lambda send: copy(src, dst, send, deep_sem(index, side, q, off), line_peers[side])
        )

    def deep_await(index, side, q, off):
        _, c0, cols, _ = outof[index]
        part = deep_slot(side, q, off, (c0, cols))
        copy(part, part, pool_ring.at[0, 0], deep_sem(index, side, q, off), partner).wait_recv()
        return part

    def line_direct(index, off):
        _, c0, cols, _ = outof[index]
        src, dst = block(0, off, (c0, cols)), line_land.at[ep, :, pl.ds(c0, cols)]
        sem = line_recv.at[lined[index]]
        side = 1 if off > 0 else -1
        send_out(valid(off), "line", side, lambda send: copy(src, dst, send, sem, (group, ep + off)))

    def block(q, off, span):
        return parts_ref.at[spot(q) * nep + ep + off, :, pl.ds(span[0], span[1])]

    def scatter_line(index, q, off):
        _, c0, cols, _ = outof[index]
        here = block(q, off, (c0, cols))
        if off != 0:
            side = 1 if off > 0 else -1
            behind = has[-side]

            @pl.when(both(valid(off), behind))
            def _():
                add(here, [here, deep_await(index, side, q, off)])

            deep_send(valid(off), index, q, off, side)
        else:
            left, right = has[-1], has[1]

            @pl.when(left & right)
            def _():
                add(here, [here, deep_await(index, 1, q, 0), deep_await(index, -1, q, 0)])

            @pl.when(left & jnp.logical_not(right))
            def _():
                add(here, [here, deep_await(index, 1, q, 0)])

            @pl.when(right & jnp.logical_not(left))
            def _():
                add(here, [here, deep_await(index, -1, q, 0)])

    def plane_terms(off, span):
        return [block(0, off, span)] + [ring_slot(side, 0, off, span) for side in (1, -1)]

    def scatter_ring(index, off, d):
        kind, c0, cols, _ = outof[index]
        whole = (c0, cols)
        split = halves(c0, cols)
        if d == far:
            for side in (1, -1):
                ring_send(valid(off), index, off, side, d, split[side])
            if far > 1:
                for side in (1, -1):
                    ring_send(valid(off), index, off, side, d - 1, split[-side])
        elif d > 0:
            when(valid(off), lambda: ring_await(index, off, d, 1 if d + 1 == far else 2))
            for side in (1, -1):
                for span in [split[side]] if d + 1 == far else [whole]:
                    def go(side=side, span=span):
                        here = block(side * d, off, span)
                        add(here, [here, ring_slot(side, d, off, span)])

                    when(valid(off), go)
                    ring_send(valid(off), index, off, side, d, span)
        else:
            when(valid(off), lambda: ring_await(index, off, 0, 1 if far == 1 else 2))
            if off != 0:
                when(valid(off), lambda: add(block(0, off, whole), plane_terms(off, whole)))
                line_direct(index, off)
            elif kind == "ring":
                add(out_ref.at[:, pl.ds(c0, cols)], plane_terms(0, whole))

    def scatter_last(index):
        _, c0, cols, _ = outof[index]
        at = pl.ds(c0, cols)
        part = line_land.at[pl.ds(0, nep - 1), :, at]
        copy(part, part, pool_line.at[0, 0], line_recv.at[lined[index]], partner).wait_recv()
        others = [line_land.at[lax.rem(ep + step, nep), :, at] for step in range(1, nep)]
        add(out_ref.at[:, at], plane_terms(0, (c0, cols)) + others)

    for what, index, q, off, d in gather_order(into, nplane, nep):
        if what == "tables":
            tables()
        elif what == "own":
            gather_own(index)
        elif what == "line":
            gather_line(index, q, off)
        elif what == "ring":
            gather_ring(index, off, d)
        elif what == "pick":
            pick(index)
        else:
            product(index, q)
    activate()
    weight_copies[2].wait()
    for what, index, q, off, d in scatter_order(outof, nplane, nep):
        if what == "down":
            down(index)
        elif what == "spread":
            spread(index)
        elif what == "ring":
            scatter_ring(index, off, d)
        elif what == "last":
            scatter_last(index)
        else:
            scatter_line(index, q, off)
    count_copy().wait_recv()
    load_ref[...] = (count_own[0] + count_in[...])[0:1, 0:2] / top
    for make in swaps:
        make().wait_send()
    for (kind, _), pool in pools.items():
        for cond, make in pool[-(pool_ring if kind == "ring" else pool_line).shape[1]:]:
            when(cond, lambda: make().wait_send())

def layer(tokens, ids, picks, gates, hot, w_gate, w_up, w_down, plan, shapes):
    nplane, nep, _, into, outof = plan
    far = nplane // 2
    count = nplane * nep
    rows, width = tokens.shape
    dma = pltpu.SemaphoreType.DMA
    vmem = pl.BlockSpec(memory_space=pltpu.VMEM)
    hbm = pl.BlockSpec(memory_space=pl.ANY)
    lines_in = sum(kind == "line" for kind, _, _, _ in into)
    lines_out = sum(kind == "line" for kind, _, _, _ in outof)
    rings_in, rings_out = len(into) - lines_in, len(outof) - lines_out
    swaps = len(into) + len(outof) + 1
    return pl.pallas_call(
        functools.partial(layer_kernel, plan),
        out_shape=[
            jax.ShapeDtypeStruct((rows, width), tokens.dtype),
            jax.ShapeDtypeStruct((1, 2), jnp.float32),
        ],
        in_specs=[pl.BlockSpec(memory_space=pltpu.SMEM), hbm, vmem, vmem, vmem, hbm, hbm, hbm],
        out_specs=[vmem, vmem],
        scratch_shapes=[pltpu.VMEM(shape, kind) for shape, kind in shapes] + [
            dma((len(into),)), dma((3,)), dma((2, POOL)), dma((2, POOL)),
            dma((len(into), far, nep)), dma((lines_in * nep + rings_in * count,)), dma((swaps,)), dma((swaps,)),
            dma((lines_out * nep + rings_out, far)), dma((lines_out,)), dma((rings_out, 2, count)),
        ],
        compiler_params=pltpu.CompilerParams(
            collective_id=2, has_side_effects=True, vmem_limit_bytes=VMEM_LIMIT
        ),
    )(hot, tokens, ids, picks, gates, w_gate, w_up, w_down)


def buffers(nplane, nep, rows, width, top, hidden, cap, kind):
    count = nplane * nep
    total = count * rows
    f32 = jnp.float32
    return [
        ((count, rows, width + 128), kind),
        ((2 * cap, total), kind), ((total, 2 * cap), kind),
        ((width, hidden), kind), ((width, hidden), kind), ((hidden, width), kind),
        ((2 * cap, width), kind), ((cap, width), kind),
        ((2 * cap, hidden), f32), ((2 * cap, hidden), f32), ((2 * cap, hidden), kind),
        ((2 * cap, width), kind), ((cap, width), kind), ((count, rows, width), kind),
        ((2, nplane // 2, nep, rows, width), kind), ((nep, rows, width), kind),
        ((2, count, rows, width), kind),
        ((2, 8, 128), f32), ((8, 128), f32),
    ]


def cuts(width, shares):
    unit = 256
    units = width // unit
    total = sum(share for _, share, _ in shares)
    made, at, seen = [], 0, 0
    for kind, share, start in shares:
        seen += share
        end = units * seen // total
        made.append((kind, at * unit, (end - at) * unit, start))
        at = end
    return tuple(made)


def body(
    tokens, expert_ids, gate_scores, replica_pick, replica_hot, gate_weight, up_weight, down_weight
):
    ngroup = lax.axis_size("group")
    nep = lax.axis_size("ep")
    nplane = ngroup // 2
    device_count = ngroup * nep
    group_index = lax.axis_index("group")
    ep_index = lax.axis_index("ep")
    core = group_index % 2
    me = group_index * nep + ep_index
    partner = (group_index + 1 - 2 * core) * nep + ep_index
    tok_dev, width = tokens.shape
    top_count = expert_ids.shape[1]
    most = (tok_dev // 2 * top_count + device_count - 1) // device_count + 1
    capacity = 2 * most * nplane * nep
    cut = width // 256 * 128
    back_cut = width * 11 // 14 // 128 * 128

    hidden = gate_weight.shape[2]
    plan_shapes = buffers(nplane, nep, tok_dev, width, top_count, hidden, capacity, tokens.dtype)
    need = sum(math.prod(shape) * jnp.dtype(kind).itemsize for shape, kind in plan_shapes)
    if nplane % 2 == 0 and nplane > 2 and device_count <= 256 and need < VMEM_LIMIT * 7 // 8:
        plan = (nplane, nep, most, cuts(width, INTO), cuts(width, OUTOF))
        return layer(
            tokens, expert_ids.T, replica_pick.T, gate_scores.T, replica_hot,
            gate_weight[0], up_weight[0], down_weight[0], plan, plan_shapes,
        )

    coded = expert_ids * (ngroup + 1) + replica_pick
    note = jnp.concatenate([coded.astype(jnp.float32), gate_scores], axis=1).reshape(-1, 128)
    every, notes = gather_plane(tokens, note, nplane, nep, cut)
    every = every.reshape(nplane * nep * tok_dev, width)
    routing = notes.reshape(device_count * tok_dev, 2 * top_count)
    coded = routing[:, :top_count].astype(jnp.int32)
    ids = coded // (ngroup + 1)
    picks = coded % (ngroup + 1)
    hot = replica_hot[ep_index]
    replicated = (ids % nep == ep_index) & (ids // nep == hot) & (picks < ngroup)
    primary_load = jnp.sum(((ids == me) & ~replicated).astype(jnp.float32))
    replica_load = jnp.sum((replicated & (picks == group_index)).astype(jnp.float32))
    loads = jnp.stack([primary_load, replica_load])[None, :] / top_count

    mine = routing.reshape(nplane, 2, nep * tok_dev, 2 * top_count)
    mine = lax.dynamic_index_in_dim(mine, core, 1, keepdims=False).reshape(-1, 2 * top_count)
    my_ids = mine[:, :top_count].astype(jnp.int32) // (ngroup + 1)
    my_gates = mine[:, top_count:]

    def spots(expert):
        chosen = my_ids == expert
        mask = jnp.any(chosen, axis=1)
        scale = jnp.sum(jnp.where(chosen, my_gates, 0.0), axis=1)
        place = jnp.where(mask, jnp.cumsum(mask.astype(jnp.int32)) - 1, -1)
        spot = place[None, :] == jnp.arange(capacity, dtype=jnp.int32)[:, None]
        return spot, jnp.sum(jnp.where(spot, scale[None, :], 0.0), axis=1)

    spot_me, scale_me = spots(me)
    spot_other, scale_other = spots(partner)
    select = jnp.concatenate([spot_me, spot_other], axis=0).astype(jnp.bfloat16)
    row_scale = jnp.concatenate([scale_me, scale_other], axis=0)
    swap = [(index, index ^ 1) for index in range(ngroup)]

    picked = jnp.dot(select, every, preferred_element_type=jnp.float32).astype(jnp.bfloat16)
    inputs = jnp.concatenate(
        [picked[:capacity], lax.ppermute(picked[capacity:], "group", swap)], axis=0
    )
    gate_act = jnp.dot(inputs, gate_weight[0], preferred_element_type=jnp.float32)
    up_act = jnp.dot(inputs, up_weight[0], preferred_element_type=jnp.float32)
    hidden = (jax.nn.silu(gate_act) * up_act).astype(jnp.bfloat16)
    pair_out = jnp.dot(hidden, down_weight[0], preferred_element_type=jnp.float32).astype(jnp.bfloat16)
    pairs = jnp.concatenate(
        [pair_out[:capacity], lax.ppermute(pair_out[capacity:], "group", swap)], axis=0
    )
    scaled = (pairs.astype(jnp.float32) * row_scale[:, None]).astype(jnp.bfloat16)
    spread = lax.dot_general(
        select, scaled, (((0,), (0,)), ((), ())), preferred_element_type=jnp.float32
    ).astype(jnp.bfloat16)
    mixed = scatter_plane(spread.reshape(nplane, nep, tok_dev, width), back_cut)
    return mixed, loads


def solution(mesh):
    rows = P(AXES, None)
    weights = P(AXES, None, None)
    return jax.shard_map(
        body,
        mesh=mesh,
        in_specs=(rows, rows, rows, rows, P(), weights, weights, weights),
        out_specs=(rows, rows),
        check_vma=False,
    )
```

```python
import functools
import math

import jax
import jax.numpy as jnp
from jax import lax
from jax.experimental import pallas as pl
from jax.experimental.pallas import tpu as pltpu
from jax.sharding import PartitionSpec as P

AXES = ("group", "ep")
MESH = pl.DeviceIdType.MESH

LINE_STEP, RING_STEP, DEEP_STEP, PRODUCT_STEP = 2.3, 6.0, 4.3, 3.1
SPREAD_STEP, BACK_RING, BACK_LINE, BACK_DEEP = 1.1, 2.0, 0.7, 3.0
BACK_LAST = 2.8
PIECES = 4
POOL = 12
INTO = (("line", 3, 1.5), ("line", 3, 1.3), ("line", 3, 10.3), ("line", 2, 11.6), ("ring", 3, 1.6))
OUTOF = (("ring", 3, 1.1), ("line", 4, 1.5), ("line", 4, 6.4), ("line", 3, 4.4))
VMEM_LIMIT = 67043328
SPARE = 3 * 2 ** 20


def place_of(nplane, nep):
    group = lax.axis_index("group")
    ep = lax.axis_index("ep")
    core = lax.rem(group, 2)
    plane = lax.div(group, 2)

    def plane_peer(step):
        other = lax.rem(plane + step, nplane)
        return other, (other * 2 + core, ep)

    def ep_peer(step):
        other = lax.rem(ep + step, nep)
        return other, (group, other)

    return plane, ep, plane_peer, ep_peer


def greet(nplane, nep, plane_peer, ep_peer):
    barrier = pltpu.get_barrier_semaphore()
    for step in range(1, nplane):
        pl.semaphore_signal(barrier, inc=1, device_id=plane_peer(step)[1], device_id_type=MESH)
    for step in range(1, nep):
        pl.semaphore_signal(barrier, inc=1, device_id=ep_peer(step)[1], device_id_type=MESH)
    pl.semaphore_wait(barrier, nplane + nep - 2)


def gather_kernel(
    nplane, nep, cut, x_ref, note_ref, out_ref, notes_ref,
    own_sem, send_a, recv_a, send_b, recv_b, right_a, left_a, right_b, left_b, note_send, note_recv,
):
    plane, ep, plane_peer, ep_peer = place_of(nplane, nep)
    group = lax.axis_index("group")
    me = group * nep + ep
    total = 2 * nplane * nep
    width = x_ref.shape[1]
    cols = {"a": pl.ds(0, cut), "b": pl.ds(cut, width - cut)}
    recv = {"a": recv_a, "b": recv_b}
    rights = {"a": right_a, "b": right_b}
    lefts = {"a": left_a, "b": left_b}
    own = pltpu.make_async_copy(x_ref, out_ref.at[plane, ep], own_sem.at[0])
    own.start()
    own_note = pltpu.make_async_copy(note_ref, notes_ref.at[me], own_sem.at[1])
    own_note.start()

    barrier = pltpu.get_barrier_semaphore()
    for step in range(1, total):
        other = lax.rem(me + step, total)
        pl.semaphore_signal(
            barrier, inc=1, device_id=(lax.div(other, nep), lax.rem(other, nep)), device_id_type=MESH
        )
    pl.semaphore_wait(barrier, total - 1)

    def copy(src, p, e, half, send, target):
        return pltpu.make_async_remote_copy(
            src_ref=src.at[:, cols[half]],
            dst_ref=out_ref.at[p, e, :, cols[half]],
            send_sem=send,
            recv_sem=recv[half].at[p * nep + e],
            device_id=target,
            device_id_type=MESH,
        )

    sends = []
    used = {"a": 0, "b": 0}

    def push(src, p, e, half):
        send = send_a if half == "a" else send_b
        for step in range(1, nplane):
            made = copy(src, p, e, half, send.at[used[half]], plane_peer(step)[1])
            used[half] += 1
            made.start()
            sends.append(made)

    def arrived(p, e, half):
        copy(out_ref.at[p, e], p, e, half, send_a.at[0], ep_peer(1)[1]).wait_recv()

    def to_right(src, p, e, half):
        return copy(src, p, e, half, rights[half].at[p * nep + e], (group, lax.rem(ep + 1, nep)))

    def to_left(src, p, e, half):
        return copy(src, p, e, half, lefts[half].at[p * nep + e], (group, lax.rem(ep + nep - 1, nep)))

    has_right, has_left = ep < nep - 1, ep > 0

    def both_ways(src, p, half):
        @pl.when(has_right)
        def _():
            to_right(src, p, ep, half).start()

        @pl.when(has_left)
        def _():
            to_left(src, p, ep, half).start()

    def chain(p, back, half):
        @pl.when(ep - back >= 0)
        def _():
            arrived(p, ep - back, half)

            @pl.when(has_right)
            def _():
                to_right(out_ref.at[p, ep - back], p, ep - back, half).start()

        @pl.when(ep + back < nep)
        def _():
            arrived(p, ep + back, half)

            @pl.when(has_left)
            def _():
                to_left(out_ref.at[p, ep + back], p, ep + back, half).start()

    def chain_end(p, back, half):
        @pl.when((ep - back >= 0) & has_right)
        def _():
            to_right(out_ref.at[p, ep - back], p, ep - back, half).wait_send()

        @pl.when((ep + back < nep) & has_left)
        def _():
            to_left(out_ref.at[p, ep + back], p, ep + back, half).wait_send()

    def note(source, step, target):
        return pltpu.make_async_remote_copy(
            src_ref=note_ref,
            dst_ref=notes_ref.at[source],
            send_sem=note_send.at[step],
            recv_sem=note_recv.at[source],
            device_id=(lax.div(target, nep), lax.rem(target, nep)),
            device_id_type=MESH,
        )

    both_ways(x_ref, plane, "a")
    push(x_ref, plane, ep, "b")
    push(x_ref, plane, ep, "a")
    both_ways(x_ref, plane, "b")
    for step in range(1, total):
        note(me, step, lax.rem(me + step, total)).start()
    for back in range(1, max(nplane, nep)):
        if back < nep:
            chain(plane, back, "a")
        if back < nplane:
            source = lax.rem(plane + nplane - back, nplane)
            arrived(source, ep, "b")
            both_ways(out_ref.at[source, ep], source, "b")
        if back < nep:
            left_in, right_in = ep - back >= 0, ep + back < nep

            @pl.when(left_in)
            def _():
                for step in range(1, nplane):
                    copy(
                        out_ref.at[plane, ep - back], plane, ep - back, "a",
                        send_a.at[(nplane - 1) * back + step - 1], plane_peer(step)[1],
                    ).start()

            @pl.when(right_in)
            def _():
                for step in range(1, nplane):
                    copy(
                        out_ref.at[plane, ep + back], plane, ep + back, "a",
                        send_a.at[(nplane - 1) * (nep + back) + step - 1], plane_peer(step)[1],
                    ).start()
    for back in range(1, nep):
        for p_back in range(nplane):
            chain(lax.rem(plane + nplane - p_back, nplane), back, "b")
    for p_back in range(1, nplane):
        p = lax.rem(plane + nplane - p_back, nplane)
        for e in range(nep):
            arrived(p, e, "a")
    for step in range(1, total):
        source = lax.rem(me + total - step, total)
        note(source, step, lax.rem(me + 1, total)).wait_recv()
    for made in sends:
        made.wait_send()
    for back in range(1, nep):
        @pl.when(ep - back >= 0)
        def _():
            for step in range(1, nplane):
                copy(
                    out_ref.at[plane, ep - back], plane, ep - back, "a",
                    send_a.at[(nplane - 1) * back + step - 1], plane_peer(step)[1],
                ).wait_send()

        @pl.when(ep + back < nep)
        def _():
            for step in range(1, nplane):
                copy(
                    out_ref.at[plane, ep + back], plane, ep + back, "a",
                    send_a.at[(nplane - 1) * (nep + back) + step - 1], plane_peer(step)[1],
                ).wait_send()

    for back in range(nep):
        for half in ("a", "b"):
            for p_back in range(nplane if half == "b" else 1):
                p = lax.rem(plane + nplane - p_back, nplane)
                if back == 0:
                    @pl.when(has_right)
                    def _():
                        to_right(x_ref, p, ep, half).wait_send()

                    @pl.when(has_left)
                    def _():
                        to_left(x_ref, p, ep, half).wait_send()
                else:
                    chain_end(p, back, half)
    for step in range(1, total):
        note(me, step, lax.rem(me + step, total)).wait_send()
    own.wait()
    own_note.wait()


def gather_plane(tokens, note, nplane, nep, cut):
    rows, width = tokens.shape
    count = nplane * nep
    dma = pltpu.SemaphoreType.DMA
    vmem = pl.BlockSpec(memory_space=pltpu.VMEM)
    return pl.pallas_call(
        functools.partial(gather_kernel, nplane, nep, cut),
        out_shape=[
            jax.ShapeDtypeStruct((nplane, nep, rows, width), tokens.dtype),
            jax.ShapeDtypeStruct((2 * count,) + note.shape, note.dtype),
        ],
        in_specs=[vmem, vmem],
        out_specs=[vmem, vmem],
        scratch_shapes=[
            dma((2,)),
            dma((2 * (nplane - 1) * nep,)), dma((count,)), dma((nplane - 1,)), dma((count,)),
            dma((count,)), dma((count,)), dma((count,)), dma((count,)),
            dma((2 * count,)), dma((2 * count,)),
        ],
        compiler_params=pltpu.CompilerParams(collective_id=0, has_side_effects=True),
    )(tokens, note)


def scatter_kernel(
    nplane, nep, cut, part_ref, out_ref,
    land_a1, land_b1, mid_a, mid_b, land_a2, land_b2,
    send_a1, recv_a1, send_b1, recv_b1, send_a2, recv_a2, send_b2, recv_b2,
):
    plane, ep, plane_peer, ep_peer = place_of(nplane, nep)
    width = out_ref.shape[1]
    cols_a, cols_b = pl.ds(0, cut), pl.ds(cut, width - cut)
    greet(nplane, nep, plane_peer, ep_peer)

    def move(src, dst, send, recv, target):
        made = pltpu.make_async_remote_copy(
            src_ref=src, dst_ref=dst, send_sem=send, recv_sem=recv, device_id=target, device_id_type=MESH
        )
        made.start()
        return made

    first_a, first_b = {}, {}
    for item in range(1, max(nplane, nep) + 1):
        if item <= nep:
            e = lax.rem(ep + item, nep)
            for step in range(1, nplane):
                p, target = plane_peer(step)
                spot = (step - 1) * nep + item - 1
                first_a[item, step] = move(
                    part_ref.at[p, e, :, cols_a], land_a1.at[step - 1, item - 1],
                    send_a1.at[spot], recv_a1.at[spot], target,
                )
        if item <= nplane:
            p = lax.rem(plane + item, nplane)
            for step in range(1, nep):
                e, target = ep_peer(step)
                spot = (step - 1) * nplane + item - 1
                first_b[item, step] = move(
                    part_ref.at[p, e, :, cols_b], land_b1.at[step - 1, item - 1],
                    send_b1.at[spot], recv_b1.at[spot], target,
                )
    second_a, second_b = [], []
    for item in range(1, max(nplane, nep) + 1):
        if item <= nep:
            e, target = ep_peer(item)
            total = part_ref[plane, e, :, cols_a].astype(jnp.float32)
            for step in range(1, nplane):
                first_a[item, step].wait_recv()
                total = total + land_a1[step - 1, item - 1].astype(jnp.float32)
            if item < nep:
                mid_a[item - 1] = total.astype(mid_a.dtype)
                second_a.append(
                    move(mid_a.at[item - 1], land_a2.at[item - 1], send_a2.at[item - 1], recv_a2.at[item - 1], target)
                )
            else:
                total_a = total
        if item <= nplane:
            p, target = plane_peer(item)
            total = part_ref[p, ep, :, cols_b].astype(jnp.float32)
            for step in range(1, nep):
                first_b[item, step].wait_recv()
                total = total + land_b1[step - 1, item - 1].astype(jnp.float32)
            if item < nplane:
                mid_b[item - 1] = total.astype(mid_b.dtype)
                second_b.append(
                    move(mid_b.at[item - 1], land_b2.at[item - 1], send_b2.at[item - 1], recv_b2.at[item - 1], target)
                )
            else:
                total_b = total
    for index, made in enumerate(second_a):
        made.wait_recv()
        total_a = total_a + land_a2[index].astype(jnp.float32)
    out_ref[:, cols_a] = total_a.astype(out_ref.dtype)
    for index, made in enumerate(second_b):
        made.wait_recv()
        total_b = total_b + land_b2[index].astype(jnp.float32)
    out_ref[:, cols_b] = total_b.astype(out_ref.dtype)
    for made in list(first_a.values()) + list(first_b.values()) + second_a + second_b:
        made.wait_send()


def scatter_plane(parts, cut):
    nplane, nep, rows, width = parts.shape
    rest = width - cut
    kind = parts.dtype
    dma = pltpu.SemaphoreType.DMA
    pairs_a, pairs_b = (nplane - 1) * nep, (nep - 1) * nplane
    return pl.pallas_call(
        functools.partial(scatter_kernel, nplane, nep, cut),
        out_shape=jax.ShapeDtypeStruct((rows, width), kind),
        in_specs=[pl.BlockSpec(memory_space=pltpu.VMEM)],
        out_specs=pl.BlockSpec(memory_space=pltpu.VMEM),
        scratch_shapes=[
            pltpu.VMEM((nplane - 1, nep, rows, cut), kind),
            pltpu.VMEM((nep - 1, nplane, rows, rest), kind),
            pltpu.VMEM((nep - 1, rows, cut), kind),
            pltpu.VMEM((nplane - 1, rows, rest), kind),
            pltpu.VMEM((nep - 1, rows, cut), kind),
            pltpu.VMEM((nplane - 1, rows, rest), kind),
            dma((pairs_a,)), dma((pairs_a,)), dma((pairs_b,)), dma((pairs_b,)),
            dma((nep - 1,)), dma((nep - 1,)), dma((nplane - 1,)), dma((nplane - 1,)),
        ],
        compiler_params=pltpu.CompilerParams(collective_id=1, has_side_effects=True),
    )(parts)


def ring_spot(nplane, index):
    half = nplane // 2
    return lax.select(index < half, 2 * index, 2 * (nplane - 1 - index) + 1)


def ring_index(nplane, plane):
    row = lax.div(plane, 2)
    return lax.select(lax.rem(plane, 2) == 0, row, nplane - 1 - row)


def offsets(nep):
    return [0] + [side * back for back in range(1, nep) for side in (-1, 1)]


def gather_order(parts, nplane, nep):
    far = nplane // 2
    events, ready = [], 0.0
    for index, (kind, _, _, start) in enumerate(parts):
        events.append((start, 0, ("own", index, 0, 0, 0)))
        last = start
        if kind == "line":
            for off in offsets(nep):
                at = start + LINE_STEP * abs(off)
                if off:
                    events.append((at, 1, ("line", index, 0, off, 0)))
                for d in range(1, far + 1):
                    last = max(last, at + RING_STEP * d)
                    events.append((at + RING_STEP * d, 1 + d, ("ring", index, 0, off, d)))
        else:
            for d in range(1, far + 1):
                events.append((start + RING_STEP * d, 1 + d, ("ring", index, 0, 0, d)))
            for q in range(nplane):
                for off in offsets(nep)[1:]:
                    at = start + RING_STEP * min(q, nplane - q) + DEEP_STEP * abs(off)
                    last = max(last, at)
                    events.append((at, 2 + far, ("line", index, q, off, 0)))
        ready = last if index == 0 else max(last, ready)
        if index == 0:
            events.append((last, 3 + far, ("tables", index, 0, 0, 0)))
        events.append((ready, 4 + far, ("pick", index, 0, 0, 0)))
        for piece in range(PIECES):
            events.append((ready + PRODUCT_STEP * (piece + 1), 5 + far, ("product", index, piece, 0, 0)))
    events.sort()
    return [event for _, _, event in events]


def scatter_order(parts, nplane, nep):
    far = nplane // 2
    events = []
    for index, (kind, _, _, start) in enumerate(parts):
        events.append((start, 0, ("down", index, 0, 0, 0)))
        begin = start + SPREAD_STEP
        events.append((begin, 1, ("spread", index, 0, 0, 0)))
        if kind == "line":
            for off in offsets(nep):
                for d in range(far, -1, -1):
                    at = begin + BACK_RING * (far - d) + BACK_LINE * (nep - 1 - abs(off))
                    events.append((at, 2 + nep - abs(off), ("ring", index, 0, off, d)))
            at = begin + BACK_RING * far + BACK_LINE * (nep - 1) + BACK_LAST
            events.append((at, 3 + nep, ("last", index, 0, 0, 0)))
        else:
            for q in range(nplane):
                for off in offsets(nep):
                    at = begin + BACK_DEEP * (nep - 1 - abs(off))
                    events.append((at, 2 + nep - abs(off), ("line", index, q, off, 0)))
            done = begin + BACK_DEEP * (nep - 1)
            for d in range(far, -1, -1):
                events.append((done + BACK_RING * (far - d), 3 + nep, ("ring", index, 0, 0, d)))
    events.sort(key=lambda event: (event[0], event[1], event[2][1], event[2][2], -event[2][3], -event[2][4]))
    return [event for _, _, event in events]


def layer_kernel(
    plan, hot_hbm, tok_ref, ids_hbm, picks_hbm, gates_hbm, wg_hbm, wu_hbm, wd_hbm, out_ref, load_ref,
    hot_ref, ids_ref, picks_ref, gates_ref, xs, sel, back, wg, wu, wd, inputs, stage, acc_g, acc_u, hidden, pairs, stage2, parts_ref,
    ring_land, line_land, deep_land, count_own, count_in,
    own_sem, small_sem, w_sem, pool_ring, pool_line, x_ring, x_line, swap_send, swap_recv, ring_recv, line_recv, deep_recv,
):
    nplane, nep, most, into, outof = plan
    far = nplane // 2
    count = nplane * nep
    rows, width = out_ref.shape
    top = ids_ref.shape[0]
    total = count * rows
    cap = stage.shape[0]
    ngroup = 2 * nplane
    group = lax.axis_index("group")
    ep = lax.axis_index("ep")
    core = lax.rem(group, 2)
    me_ring = ring_index(nplane, lax.div(group, 2))
    partner_group = group + 1 - 2 * core
    partner = (partner_group, ep)
    f32 = jnp.float32
    bf16 = jnp.bfloat16

    def spot(q):
        return lax.rem(me_ring + q + nplane, nplane)

    def ring_peer(side):
        return (ring_spot(nplane, spot(side)) * 2 + core, ep)

    peers = {1: ring_peer(1), -1: ring_peer(-1)}
    line_peers = {1: (group, lax.min(ep + 1, nep - 1)), -1: (group, lax.max(ep - 1, 0))}
    has = {1: ep < nep - 1, -1: ep > 0}

    def valid(off):
        if off == 0:
            return None
        return (ep + off < nep) if off > 0 else (ep + off >= 0)

    def both(a, b):
        if a is None:
            return b
        return a if b is None else a & b

    def when(cond, run):
        if cond is None:
            run()
        else:
            pl.when(cond)(run)

    pools = {key: [] for key in (("ring", 1), ("ring", -1), ("line", 1), ("line", -1))}
    swaps = []

    def copy(src, dst, send, recv, target):
        return pltpu.make_async_remote_copy(
            src_ref=src, dst_ref=dst, send_sem=send, recv_sem=recv, device_id=target, device_id_type=MESH
        )

    def send_out(cond, kind, side, make):
        pool = pools[kind, side]
        sems = (pool_ring if kind == "ring" else pool_line).at[0 if side > 0 else 1]
        turn = len(pool) % sems.shape[0]
        if len(pool) >= sems.shape[0]:
            old_cond, old = pool[-sems.shape[0]]
            when(old_cond, lambda: old().wait_send())

        def ready():
            return make(sems.at[turn])

        when(cond, lambda: ready().start())
        pool.append((cond, ready))

    def swap(make):
        make().start()
        swaps.append(make)

    lead = xs.shape[2] - width
    own_block = me_ring * nep + ep
    small_copies = []
    for index, (src, dst) in enumerate(
        ((ids_hbm, ids_ref), (picks_hbm, picks_ref), (gates_hbm, gates_ref), (hot_hbm, hot_ref))
    ):
        made = pltpu.make_async_copy(src, dst, small_sem.at[index])
        made.start()
        small_copies.append(made)
    own_copies = []
    for index, (_, c0, cols, _) in enumerate(into):
        made = pltpu.make_async_copy(
            tok_ref.at[:, pl.ds(c0, cols)], xs.at[own_block, :, pl.ds(lead + c0, cols)], own_sem.at[index]
        )
        made.start()
        own_copies.append(made)
    weight_copies = []
    for index, (src, dst) in enumerate(((wg_hbm, wg), (wu_hbm, wu), (wd_hbm, wd))):
        made = pltpu.make_async_copy(src, dst, w_sem.at[index])
        made.start()
        weight_copies.append(made)

    barrier = pltpu.get_barrier_semaphore()
    for target in (partner, peers[1], peers[-1]):
        pl.semaphore_signal(barrier, inc=1, device_id=target, device_id_type=MESH)
    for side in (1, -1):
        @pl.when(has[side])
        def _(side=side):
            pl.semaphore_signal(barrier, inc=1, device_id=line_peers[side], device_id_type=MESH)

    for made in small_copies:
        made.wait()
    own = jnp.concatenate(
        [ids_ref[...].astype(f32), picks_ref[...].astype(f32), gates_ref[...]], axis=0
    )
    own = jnp.concatenate([own, jnp.zeros((3 * top, lead - rows), f32)], axis=1)
    own = jnp.concatenate([own, jnp.zeros((lead - 3 * top, lead), f32)], axis=0)
    xs[own_block, :, pl.ds(0, lead)] = own.T[:rows].astype(bf16)
    pl.semaphore_wait(barrier, 3 + has[1].astype(jnp.int32) + has[-1].astype(jnp.int32))

    def span_of(index):
        _, c0, cols, _ = into[index]
        return (0, lead + cols) if c0 == 0 else (lead + c0, cols)

    def x_launch(cond, sem, kind, side, block, cols, target):
        part = xs.at[block, :, pl.ds(cols[0], cols[1])]
        send_out(cond, kind, side, lambda send: copy(part, part, send, sem, target))

    def x_wait(sem, blocks, cols):
        part = xs.at[pl.ds(0, blocks), :, pl.ds(cols[0], cols[1])]
        copy(part, part, pool_ring.at[0, 0], sem, partner).wait_recv()

    def halves(c0, cols):
        low = cols // 256 * 128
        return {1: (c0, low), -1: (c0 + low, cols - low)}

    starts_x = [0]
    for kind, _, _, _ in into:
        starts_x.append(starts_x[-1] + (nep if kind == "line" else count))

    def line_sem(index, q, off):
        at = starts_x[index] + ep + off
        return x_line.at[at if into[index][0] == "line" else at + spot(q) * nep]

    def ring_out(cond, index, block, off, side, d):
        span = span_of(index) if d < far else halves(*span_of(index))[side]
        x_launch(cond, x_ring.at[index, d - 1, ep + off], "ring", side, block, span, peers[side])

    def line_out(index, q, off, side):
        cond = both(valid(off), has[side])
        block = spot(q) * nep + ep + off
        x_launch(cond, line_sem(index, q, off), "line", side, block, span_of(index), line_peers[side])

    def gather_own(index):
        own_copies[index].wait()
        for side in (1, -1):
            line_out(index, 0, 0, side)
        for side in (1, -1):
            ring_out(None, index, own_block, 0, side, 1)

    def gather_line(index, q, off):
        block = spot(q) * nep + ep + off
        when(valid(off), lambda: x_wait(line_sem(index, q, off), 1, span_of(index)))
        line_out(index, q, off, 1 if off < 0 else -1)
        if into[index][0] == "line":
            for side in (1, -1):
                ring_out(valid(off), index, block, off, side, 1)

    def gather_ring(index, off, d):
        sem = x_ring.at[index, d - 1, ep + off]
        when(valid(off), lambda: x_wait(sem, 2 if d < far else 1, span_of(index)))
        for side in (1, -1):
            if d < far:
                block = spot(-side * d) * nep + ep + off
                ring_out(valid(off), index, block, off, side, d + 1)
                if into[index][0] == "ring":
                    for way in (1, -1):
                        line_out(index, -side * d, 0, way)
        if d == far and into[index][0] == "ring":
            for way in (1, -1):
                line_out(index, far, 0, way)

    def tables():
        expert = group * nep + ep
        other = partner_group * nep + ep
        hot = (hot_ref[ep] * nep + ep).astype(f32)
        expert_f, other_f = expert.astype(f32), other.astype(f32)
        block_rows = rows // 2
        a = lax.broadcasted_iota(jnp.int32, (128, 128), 0)
        b = lax.broadcasted_iota(jnp.int32, (128, 128), 1)
        before = ((lax.div(a, block_rows) == lax.div(b, block_rows)) & (a < b)).astype(f32)
        sub = lax.broadcasted_iota(jnp.int32, (8, 128), 0)
        lane8 = lax.broadcasted_iota(jnp.int32, (8, 128), 1)
        slot = lax.broadcasted_iota(jnp.int32, (cap, 128), 0).astype(f32)
        sums = [jnp.zeros((1, 1), f32) for _ in range(4)]

        def add_up(flag):
            return jnp.sum(jnp.sum(flag.astype(f32), axis=1, keepdims=True), axis=0, keepdims=True)

        for chunk in range(total // 128):
            at = pl.ds(chunk * 128, 128)
            fit = 128 // rows
            tile = xs[pl.ds(chunk * fit, fit), :, pl.ds(0, lead)].reshape(128, lead).astype(f32).T
            ids, picks, gates = tile[:top], tile[top:2 * top], tile[2 * top:3 * top]
            chosen = [ids == expert_f, ids == other_f]
            flag = [jnp.sum(c.astype(f32), axis=0, keepdims=True) for c in chosen]
            scale = [jnp.sum(jnp.where(c, gates, 0.0), axis=0, keepdims=True) for c in chosen]
            stacked = jnp.where(sub == 0, flag[0], jnp.where(sub == 1, flag[1], 0.0))
            rank = jnp.dot(stacked, before, preferred_element_type=f32)
            first = (lax.div(lane8[0:1], block_rows) + chunk * (128 // block_rows)).astype(f32) * most
            scaled = []
            for which in range(2):
                position = jnp.where(flag[which] > 0, first + rank[which:which + 1], -1.0)
                one = (slot == position).astype(f32)
                sel[pl.ds(which * cap, cap), at] = one.astype(bf16)
                scaled.append(one * scale[which])
            back[at, :] = jnp.concatenate(scaled, axis=0).T.astype(bf16)
            copied = (ids == hot) & (picks < ngroup)
            for which, (here, its) in enumerate(((expert_f, group), (other_f, partner_group))):
                sums[2 * which] = sums[2 * which] + add_up((ids == here) & ~copied)
                sums[2 * which + 1] = sums[2 * which + 1] + add_up(copied & (picks == its.astype(f32)))
        lane_n = lane8
        count_own[0] = jnp.where(lane_n == 0, sums[0], jnp.where(lane_n == 1, sums[1], 0.0))
        count_own[1] = jnp.where(lane_n == 0, sums[2], jnp.where(lane_n == 1, sums[3], 0.0))
        swap(count_copy)

    def count_copy():
        spare = len(into) + len(outof)
        return copy(count_own.at[1], count_in, swap_send.at[spare], swap_recv.at[spare], partner)

    step = 256

    def in_copy(index):
        _, c0, cols, _ = into[index]
        return copy(
            stage.at[:, pl.ds(c0, cols)], inputs.at[pl.ds(cap, cap), pl.ds(c0, cols)],
            swap_send.at[index], swap_recv.at[index], partner,
        )

    def pick(index):
        _, c0, cols, _ = into[index]

        def part(i, _):
            at = pl.ds(pl.multiple_of(c0 + i * step, step), step)
            here = pl.ds(pl.multiple_of(lead + c0 + i * step, 128), step)
            got = jnp.dot(sel[...], xs[:, :, here].reshape(total, step), preferred_element_type=f32).astype(bf16)
            inputs[pl.ds(0, cap), at] = got[:cap]
            stage[:, at] = got[cap:]
            return 0

        lax.fori_loop(0, cols // step, part, 0)
        swap(lambda: in_copy(index))

    seen = []

    def product(index, piece):
        _, c0, cols, _ = into[index]
        if piece == 0:
            in_copy(index).wait_recv()
            if not seen:
                weight_copies[0].wait()
                weight_copies[1].wait()
        first = piece not in seen
        seen.append(piece)
        last = seen.count(piece) == len(into)
        tiles = acc_g.shape[1] // step // PIECES

        def part(j, _):
            at = pl.ds(pl.multiple_of((piece * tiles + j) * step, step), step)
            acts = []
            for weight, acc in ((wg, acc_g), (wu, acc_u)):
                got = jnp.dot(
                    inputs[:, pl.ds(c0, cols)], weight[pl.ds(c0, cols), at], preferred_element_type=f32
                )
                acts.append(got if first else acc[:, at] + got)
            if last:
                hidden[:, at] = (acts[0] / (1.0 + jnp.exp(-acts[0])) * acts[1]).astype(bf16)
            else:
                acc_g[:, at], acc_u[:, at] = acts
            return 0

        lax.fori_loop(0, tiles, part, 0)

    def back_copy(index):
        _, c0, cols, _ = outof[index]
        spot_of = len(into) + index
        return copy(
            stage2.at[:, pl.ds(c0, cols)], pairs.at[pl.ds(cap, cap), pl.ds(c0, cols)],
            swap_send.at[spot_of], swap_recv.at[spot_of], partner,
        )

    def down(index):
        _, c0, cols, _ = outof[index]

        def part(i, _):
            at = pl.ds(pl.multiple_of(c0 + i * step, step), step)
            got = jnp.dot(hidden[...], wd[:, at], preferred_element_type=f32).astype(bf16)
            pairs[pl.ds(0, cap), at] = got[:cap]
            stage2[:, at] = got[cap:]
            return 0

        lax.fori_loop(0, cols // step, part, 0)
        swap(lambda: back_copy(index))

    def spread(index):
        _, c0, cols, _ = outof[index]
        back_copy(index).wait_recv()

        def part(i, _):
            at = pl.ds(pl.multiple_of(c0 + i * step, step), step)
            got = jnp.dot(back[...], pairs[:, at], preferred_element_type=f32).astype(bf16)
            parts_ref[:, :, at] = got.reshape(count, rows, step)
            return 0

        lax.fori_loop(0, cols // step, part, 0)

    def add(dst, sources):
        def part(i, _):
            at = pl.ds(pl.multiple_of(i * 16, 16), 16)
            value = sources[0][at, :].astype(f32)
            for source in sources[1:]:
                value = value + source[at, :].astype(f32)
            dst[at, :] = value.astype(dst.dtype)
            return 0

        lax.fori_loop(0, rows // 16, part, 0)

    def way(side):
        return 0 if side > 0 else 1

    starts_r = [0]
    for kind, _, _, _ in outof:
        starts_r.append(starts_r[-1] + (nep if kind == "line" else 1))

    def ring_sem(index, d, off):
        return ring_recv.at[starts_r[index] + (ep + off if outof[index][0] == "line" else 0), d]

    def ring_slot(side, d, off, span):
        return ring_land.at[way(side), d, ep + off, :, pl.ds(span[0], span[1])]

    def ring_send(cond, index, off, side, d, span):
        dst = ring_slot(side, d - 1, off, span)
        src = block(side * d, off, span)
        send_out(
            cond, "ring", side, lambda send: copy(src, dst, send, ring_sem(index, d - 1, off), peers[side])
        )

    def ring_await(index, off, d, blocks):
        _, c0, cols, _ = outof[index]
        part = ring_land.at[0, 0, pl.ds(0, blocks), :, pl.ds(c0, cols)]
        copy(part, part, pool_ring.at[0, 0], ring_sem(index, d, off), partner).wait_recv()

    def deep_slot(side, q, off, span):
        return deep_land.at[way(side), spot(q) * nep + ep + off, :, pl.ds(span[0], span[1])]

    def deep_sem(index, side, q, off):
        return deep_recv.at[deep_of[index], way(side), spot(q) * nep + ep + off]

    deep_of, lined = {}, {}
    for index, (kind, _, _, _) in enumerate(outof):
        if kind == "line":
            lined[index] = len(lined)
        else:
            deep_of[index] = len(deep_of)

    def deep_send(cond, index, q, off, side):
        _, c0, cols, _ = outof[index]
        src, dst = block(q, off, (c0, cols)), deep_slot(side, q, off, (c0, cols))
        send_out(
            cond, "line", side, lambda send: copy(src, dst, send, deep_sem(index, side, q, off), line_peers[side])
        )

    def deep_await(index, side, q, off):
        _, c0, cols, _ = outof[index]
        part = deep_slot(side, q, off, (c0, cols))
        copy(part, part, pool_ring.at[0, 0], deep_sem(index, side, q, off), partner).wait_recv()
        return part

    def line_direct(index, off):
        _, c0, cols, _ = outof[index]
        src, dst = block(0, off, (c0, cols)), line_land.at[ep, :, pl.ds(c0, cols)]
        sem = line_recv.at[lined[index]]
        side = 1 if off > 0 else -1
        send_out(valid(off), "line", side, lambda send: copy(src, dst, send, sem, (group, ep + off)))

    def block(q, off, span):
        return parts_ref.at[spot(q) * nep + ep + off, :, pl.ds(span[0], span[1])]

    def scatter_line(index, q, off):
        _, c0, cols, _ = outof[index]
        here = block(q, off, (c0, cols))
        if off != 0:
            side = 1 if off > 0 else -1
            behind = has[-side]

            @pl.when(both(valid(off), behind))
            def _():
                add(here, [here, deep_await(index, side, q, off)])

            deep_send(valid(off), index, q, off, side)
        else:
            left, right = has[-1], has[1]

            @pl.when(left & right)
            def _():
                add(here, [here, deep_await(index, 1, q, 0), deep_await(index, -1, q, 0)])

            @pl.when(left & jnp.logical_not(right))
            def _():
                add(here, [here, deep_await(index, 1, q, 0)])

            @pl.when(right & jnp.logical_not(left))
            def _():
                add(here, [here, deep_await(index, -1, q, 0)])

    def plane_terms(off, span):
        return [block(0, off, span)] + [ring_slot(side, 0, off, span) for side in (1, -1)]

    def scatter_ring(index, off, d):
        kind, c0, cols, _ = outof[index]
        whole = (c0, cols)
        split = halves(c0, cols)
        if d == far:
            for side in (1, -1):
                ring_send(valid(off), index, off, side, d, split[side])
            if far > 1:
                for side in (1, -1):
                    ring_send(valid(off), index, off, side, d - 1, split[-side])
        elif d > 0:
            when(valid(off), lambda: ring_await(index, off, d, 1 if d + 1 == far else 2))
            for side in (1, -1):
                for span in [split[side]] if d + 1 == far else [whole]:
                    def go(side=side, span=span):
                        here = block(side * d, off, span)
                        add(here, [here, ring_slot(side, d, off, span)])

                    when(valid(off), go)
                    ring_send(valid(off), index, off, side, d, span)
        else:
            when(valid(off), lambda: ring_await(index, off, 0, 1 if far == 1 else 2))
            if off != 0:
                when(valid(off), lambda: add(block(0, off, whole), plane_terms(off, whole)))
                line_direct(index, off)
            elif kind == "ring":
                add(out_ref.at[:, pl.ds(c0, cols)], plane_terms(0, whole))

    def scatter_last(index):
        _, c0, cols, _ = outof[index]
        at = pl.ds(c0, cols)
        part = line_land.at[pl.ds(0, nep - 1), :, at]
        copy(part, part, pool_line.at[0, 0], line_recv.at[lined[index]], partner).wait_recv()
        others = [line_land.at[lax.rem(ep + step, nep), :, at] for step in range(1, nep)]
        add(out_ref.at[:, at], plane_terms(0, (c0, cols)) + others)

    for what, index, q, off, d in gather_order(into, nplane, nep):
        if what == "tables":
            tables()
        elif what == "own":
            gather_own(index)
        elif what == "line":
            gather_line(index, q, off)
        elif what == "ring":
            gather_ring(index, off, d)
        elif what == "pick":
            pick(index)
        else:
            product(index, q)
    weight_copies[2].wait()
    for what, index, q, off, d in scatter_order(outof, nplane, nep):
        if what == "down":
            down(index)
        elif what == "spread":
            spread(index)
        elif what == "ring":
            scatter_ring(index, off, d)
        elif what == "last":
            scatter_last(index)
        else:
            scatter_line(index, q, off)
    count_copy().wait_recv()
    load_ref[...] = (count_own[0] + count_in[...])[0:1, 0:2] / top
    for make in swaps:
        make().wait_send()
    for (kind, _), pool in pools.items():
        for cond, make in pool[-(pool_ring if kind == "ring" else pool_line).shape[1]:]:
            when(cond, lambda: make().wait_send())

def finish_kernel(mixed_in, load_in, mixed_out, load_out, mixed_here, load_here, sems):
    trips = ((mixed_in, mixed_here, mixed_out), (load_in, load_here, load_out))
    for way in range(2):
        made = []
        for index, trip in enumerate(trips):
            made.append(pltpu.make_async_copy(trip[way], trip[way + 1], sems.at[way, index]))
            made[-1].start()
        for one in made:
            one.wait()


def layer(tokens, ids, picks, gates, hot, w_gate, w_up, w_down, plan, shapes, need):
    nplane, nep, _, into, outof = plan
    far = nplane // 2
    count = nplane * nep
    rows, width = tokens.shape
    dma = pltpu.SemaphoreType.DMA
    vmem = pl.BlockSpec(memory_space=pltpu.VMEM)
    hbm = pl.BlockSpec(memory_space=pltpu.HBM)
    lines_in = sum(kind == "line" for kind, _, _, _ in into)
    lines_out = sum(kind == "line" for kind, _, _, _ in outof)
    rings_in, rings_out = len(into) - lines_in, len(outof) - lines_out
    swaps = len(into) + len(outof) + 1
    mixed, loads = pl.pallas_call(
        functools.partial(layer_kernel, plan),
        out_shape=[
            jax.ShapeDtypeStruct((rows, width), tokens.dtype),
            jax.ShapeDtypeStruct((1, 2), jnp.float32),
        ],
        in_specs=[hbm] * 8,
        out_specs=[vmem, vmem],
        scratch_shapes=[pltpu.SMEM(hot.shape, hot.dtype)] + [
            pltpu.VMEM(x.shape, x.dtype) for x in (ids, picks, gates)
        ] + [pltpu.VMEM(shape, kind) for shape, kind in shapes] + [
            dma((len(into),)), dma((4,)), dma((3,)), dma((2, POOL)), dma((2, POOL)),
            dma((len(into), far, nep)), dma((lines_in * nep + rings_in * count,)), dma((swaps,)), dma((swaps,)),
            dma((lines_out * nep + rings_out, far)), dma((lines_out,)), dma((rings_out, 2, count)),
        ],
        compiler_params=pltpu.CompilerParams(
            collective_id=2, has_side_effects=True, vmem_limit_bytes=VMEM_LIMIT
        ),
    )(hot, tokens, ids, picks, gates, w_gate, w_up, w_down)
    return pl.pallas_call(
        finish_kernel,
        out_shape=[jax.ShapeDtypeStruct(x.shape, x.dtype) for x in (mixed, loads)],
        in_specs=[hbm, hbm],
        out_specs=[hbm, hbm],
        scratch_shapes=[pltpu.VMEM(x.shape, x.dtype) for x in (mixed, loads)] + [dma((2, 2))],
        compiler_params=pltpu.CompilerParams(vmem_limit_bytes=VMEM_LIMIT),
    )(mixed, loads)


def buffers(nplane, nep, rows, width, top, hidden, cap, kind):
    count = nplane * nep
    total = count * rows
    f32 = jnp.float32
    return [
        ((count, rows, width + 128), kind),
        ((2 * cap, total), kind), ((total, 2 * cap), kind),
        ((width, hidden), kind), ((width, hidden), kind), ((hidden, width), kind),
        ((2 * cap, width), kind), ((cap, width), kind),
        ((2 * cap, hidden), f32), ((2 * cap, hidden), f32), ((2 * cap, hidden), kind),
        ((2 * cap, width), kind), ((cap, width), kind), ((count, rows, width), kind),
        ((2, nplane // 2, nep, rows, width), kind), ((nep, rows, width), kind),
        ((2, count, rows, width), kind),
        ((2, 8, 128), f32), ((8, 128), f32),
    ]


def cuts(width, shares):
    unit = 256
    units = width // unit
    total = sum(share for _, share, _ in shares)
    made, at, seen = [], 0, 0
    for kind, share, start in shares:
        seen += share
        end = units * seen // total
        made.append((kind, at * unit, (end - at) * unit, start))
        at = end
    return tuple(made)


def body(
    tokens, expert_ids, gate_scores, replica_pick, replica_hot, gate_weight, up_weight, down_weight
):
    ngroup = lax.axis_size("group")
    nep = lax.axis_size("ep")
    nplane = ngroup // 2
    device_count = ngroup * nep
    group_index = lax.axis_index("group")
    ep_index = lax.axis_index("ep")
    core = group_index % 2
    me = group_index * nep + ep_index
    partner = (group_index + 1 - 2 * core) * nep + ep_index
    tok_dev, width = tokens.shape
    top_count = expert_ids.shape[1]
    most = (tok_dev // 2 * top_count + device_count - 1) // device_count + 1
    capacity = 2 * most * nplane * nep
    cut = width // 256 * 128
    back_cut = width * 11 // 14 // 128 * 128

    hidden = gate_weight.shape[2]
    plan_shapes = buffers(nplane, nep, tok_dev, width, top_count, hidden, capacity, tokens.dtype)
    need = sum(math.prod(shape) * jnp.dtype(kind).itemsize for shape, kind in plan_shapes)
    if nplane % 2 == 0 and nplane > 2 and device_count <= 256 and need < VMEM_LIMIT * 7 // 8:
        plan = (nplane, nep, most, cuts(width, INTO), cuts(width, OUTOF))
        return layer(
            tokens, expert_ids.T, replica_pick.T, gate_scores.T, replica_hot,
            gate_weight[0], up_weight[0], down_weight[0], plan, plan_shapes, need,
        )

    coded = expert_ids * (ngroup + 1) + replica_pick
    note = jnp.concatenate([coded.astype(jnp.float32), gate_scores], axis=1).reshape(-1, 128)
    every, notes = gather_plane(tokens, note, nplane, nep, cut)
    every = every.reshape(nplane * nep * tok_dev, width)
    routing = notes.reshape(device_count * tok_dev, 2 * top_count)
    coded = routing[:, :top_count].astype(jnp.int32)
    ids = coded // (ngroup + 1)
    picks = coded % (ngroup + 1)
    hot = replica_hot[ep_index]
    replicated = (ids % nep == ep_index) & (ids // nep == hot) & (picks < ngroup)
    primary_load = jnp.sum(((ids == me) & ~replicated).astype(jnp.float32))
    replica_load = jnp.sum((replicated & (picks == group_index)).astype(jnp.float32))
    loads = jnp.stack([primary_load, replica_load])[None, :] / top_count

    mine = routing.reshape(nplane, 2, nep * tok_dev, 2 * top_count)
    mine = lax.dynamic_index_in_dim(mine, core, 1, keepdims=False).reshape(-1, 2 * top_count)
    my_ids = mine[:, :top_count].astype(jnp.int32) // (ngroup + 1)
    my_gates = mine[:, top_count:]

    def spots(expert):
        chosen = my_ids == expert
        mask = jnp.any(chosen, axis=1)
        scale = jnp.sum(jnp.where(chosen, my_gates, 0.0), axis=1)
        place = jnp.where(mask, jnp.cumsum(mask.astype(jnp.int32)) - 1, -1)
        spot = place[None, :] == jnp.arange(capacity, dtype=jnp.int32)[:, None]
        return spot, jnp.sum(jnp.where(spot, scale[None, :], 0.0), axis=1)

    spot_me, scale_me = spots(me)
    spot_other, scale_other = spots(partner)
    select = jnp.concatenate([spot_me, spot_other], axis=0).astype(jnp.bfloat16)
    row_scale = jnp.concatenate([scale_me, scale_other], axis=0)
    swap = [(index, index ^ 1) for index in range(ngroup)]

    picked = jnp.dot(select, every, preferred_element_type=jnp.float32).astype(jnp.bfloat16)
    inputs = jnp.concatenate(
        [picked[:capacity], lax.ppermute(picked[capacity:], "group", swap)], axis=0
    )
    gate_act = jnp.dot(inputs, gate_weight[0], preferred_element_type=jnp.float32)
    up_act = jnp.dot(inputs, up_weight[0], preferred_element_type=jnp.float32)
    hidden = (jax.nn.silu(gate_act) * up_act).astype(jnp.bfloat16)
    pair_out = jnp.dot(hidden, down_weight[0], preferred_element_type=jnp.float32).astype(jnp.bfloat16)
    pairs = jnp.concatenate(
        [pair_out[:capacity], lax.ppermute(pair_out[capacity:], "group", swap)], axis=0
    )
    scaled = (pairs.astype(jnp.float32) * row_scale[:, None]).astype(jnp.bfloat16)
    spread = lax.dot_general(
        select, scaled, (((0,), (0,)), ((), ())), preferred_element_type=jnp.float32
    ).astype(jnp.bfloat16)
    mixed = scatter_plane(spread.reshape(nplane, nep, tok_dev, width), back_cut)
    return mixed, loads


def solution(mesh):
    rows = P(AXES, None)
    weights = P(AXES, None, None)
    return jax.shard_map(
        body,
        mesh=mesh,
        in_specs=(rows, rows, rows, rows, P(), weights, weights, weights),
        out_specs=(rows, rows),
        check_vma=False,
    )
```

```python
import functools
import math

import jax
import jax.numpy as jnp
from jax import lax
from jax.experimental import pallas as pl
from jax.experimental.pallas import tpu as pltpu
from jax.sharding import PartitionSpec as P

AXES = ("group", "ep")
MESH = pl.DeviceIdType.MESH

LINE_STEP, RING_STEP, DEEP_STEP, PRODUCT_STEP = 2.3, 6.0, 4.3, 3.1
SPREAD_STEP, BACK_RING, BACK_LINE, BACK_DEEP = 1.1, 2.0, 0.7, 3.0
BACK_LAST = 2.8
PIECES = 4
STRIP, PICK_STEP = 256, 0.8
POOL = 12
INTO = (("line", 3, 1.5), ("line", 3, 1.3), ("line", 3, 10.3), ("line", 2, 11.6), ("ring", 3, 1.6))
OUTOF = (("ring", 3, 1.1), ("line", 4, 1.5), ("line", 4, 6.4), ("line", 3, 4.4))
VMEM_LIMIT = 67043328
SPARE = 3 * 2 ** 20


def place_of(nplane, nep):
    group = lax.axis_index("group")
    ep = lax.axis_index("ep")
    core = lax.rem(group, 2)
    plane = lax.div(group, 2)

    def plane_peer(step):
        other = lax.rem(plane + step, nplane)
        return other, (other * 2 + core, ep)

    def ep_peer(step):
        other = lax.rem(ep + step, nep)
        return other, (group, other)

    return plane, ep, plane_peer, ep_peer


def greet(nplane, nep, plane_peer, ep_peer):
    barrier = pltpu.get_barrier_semaphore()
    for step in range(1, nplane):
        pl.semaphore_signal(barrier, inc=1, device_id=plane_peer(step)[1], device_id_type=MESH)
    for step in range(1, nep):
        pl.semaphore_signal(barrier, inc=1, device_id=ep_peer(step)[1], device_id_type=MESH)
    pl.semaphore_wait(barrier, nplane + nep - 2)


def gather_kernel(
    nplane, nep, cut, x_ref, note_ref, out_ref, notes_ref,
    own_sem, send_a, recv_a, send_b, recv_b, right_a, left_a, right_b, left_b, note_send, note_recv,
):
    plane, ep, plane_peer, ep_peer = place_of(nplane, nep)
    group = lax.axis_index("group")
    me = group * nep + ep
    total = 2 * nplane * nep
    width = x_ref.shape[1]
    cols = {"a": pl.ds(0, cut), "b": pl.ds(cut, width - cut)}
    recv = {"a": recv_a, "b": recv_b}
    rights = {"a": right_a, "b": right_b}
    lefts = {"a": left_a, "b": left_b}
    own = pltpu.make_async_copy(x_ref, out_ref.at[plane, ep], own_sem.at[0])
    own.start()
    own_note = pltpu.make_async_copy(note_ref, notes_ref.at[me], own_sem.at[1])
    own_note.start()

    barrier = pltpu.get_barrier_semaphore()
    for step in range(1, total):
        other = lax.rem(me + step, total)
        pl.semaphore_signal(
            barrier, inc=1, device_id=(lax.div(other, nep), lax.rem(other, nep)), device_id_type=MESH
        )
    pl.semaphore_wait(barrier, total - 1)

    def copy(src, p, e, half, send, target):
        return pltpu.make_async_remote_copy(
            src_ref=src.at[:, cols[half]],
            dst_ref=out_ref.at[p, e, :, cols[half]],
            send_sem=send,
            recv_sem=recv[half].at[p * nep + e],
            device_id=target,
            device_id_type=MESH,
        )

    sends = []
    used = {"a": 0, "b": 0}

    def push(src, p, e, half):
        send = send_a if half == "a" else send_b
        for step in range(1, nplane):
            made = copy(src, p, e, half, send.at[used[half]], plane_peer(step)[1])
            used[half] += 1
            made.start()
            sends.append(made)

    def arrived(p, e, half):
        copy(out_ref.at[p, e], p, e, half, send_a.at[0], ep_peer(1)[1]).wait_recv()

    def to_right(src, p, e, half):
        return copy(src, p, e, half, rights[half].at[p * nep + e], (group, lax.rem(ep + 1, nep)))

    def to_left(src, p, e, half):
        return copy(src, p, e, half, lefts[half].at[p * nep + e], (group, lax.rem(ep + nep - 1, nep)))

    has_right, has_left = ep < nep - 1, ep > 0

    def both_ways(src, p, half):
        @pl.when(has_right)
        def _():
            to_right(src, p, ep, half).start()

        @pl.when(has_left)
        def _():
            to_left(src, p, ep, half).start()

    def chain(p, back, half):
        @pl.when(ep - back >= 0)
        def _():
            arrived(p, ep - back, half)

            @pl.when(has_right)
            def _():
                to_right(out_ref.at[p, ep - back], p, ep - back, half).start()

        @pl.when(ep + back < nep)
        def _():
            arrived(p, ep + back, half)

            @pl.when(has_left)
            def _():
                to_left(out_ref.at[p, ep + back], p, ep + back, half).start()

    def chain_end(p, back, half):
        @pl.when((ep - back >= 0) & has_right)
        def _():
            to_right(out_ref.at[p, ep - back], p, ep - back, half).wait_send()

        @pl.when((ep + back < nep) & has_left)
        def _():
            to_left(out_ref.at[p, ep + back], p, ep + back, half).wait_send()

    def note(source, step, target):
        return pltpu.make_async_remote_copy(
            src_ref=note_ref,
            dst_ref=notes_ref.at[source],
            send_sem=note_send.at[step],
            recv_sem=note_recv.at[source],
            device_id=(lax.div(target, nep), lax.rem(target, nep)),
            device_id_type=MESH,
        )

    both_ways(x_ref, plane, "a")
    push(x_ref, plane, ep, "b")
    push(x_ref, plane, ep, "a")
    both_ways(x_ref, plane, "b")
    for step in range(1, total):
        note(me, step, lax.rem(me + step, total)).start()
    for back in range(1, max(nplane, nep)):
        if back < nep:
            chain(plane, back, "a")
        if back < nplane:
            source = lax.rem(plane + nplane - back, nplane)
            arrived(source, ep, "b")
            both_ways(out_ref.at[source, ep], source, "b")
        if back < nep:
            left_in, right_in = ep - back >= 0, ep + back < nep

            @pl.when(left_in)
            def _():
                for step in range(1, nplane):
                    copy(
                        out_ref.at[plane, ep - back], plane, ep - back, "a",
                        send_a.at[(nplane - 1) * back + step - 1], plane_peer(step)[1],
                    ).start()

            @pl.when(right_in)
            def _():
                for step in range(1, nplane):
                    copy(
                        out_ref.at[plane, ep + back], plane, ep + back, "a",
                        send_a.at[(nplane - 1) * (nep + back) + step - 1], plane_peer(step)[1],
                    ).start()
    for back in range(1, nep):
        for p_back in range(nplane):
            chain(lax.rem(plane + nplane - p_back, nplane), back, "b")
    for p_back in range(1, nplane):
        p = lax.rem(plane + nplane - p_back, nplane)
        for e in range(nep):
            arrived(p, e, "a")
    for step in range(1, total):
        source = lax.rem(me + total - step, total)
        note(source, step, lax.rem(me + 1, total)).wait_recv()
    for made in sends:
        made.wait_send()
    for back in range(1, nep):
        @pl.when(ep - back >= 0)
        def _():
            for step in range(1, nplane):
                copy(
                    out_ref.at[plane, ep - back], plane, ep - back, "a",
                    send_a.at[(nplane - 1) * back + step - 1], plane_peer(step)[1],
                ).wait_send()

        @pl.when(ep + back < nep)
        def _():
            for step in range(1, nplane):
                copy(
                    out_ref.at[plane, ep + back], plane, ep + back, "a",
                    send_a.at[(nplane - 1) * (nep + back) + step - 1], plane_peer(step)[1],
                ).wait_send()

    for back in range(nep):
        for half in ("a", "b"):
            for p_back in range(nplane if half == "b" else 1):
                p = lax.rem(plane + nplane - p_back, nplane)
                if back == 0:
                    @pl.when(has_right)
                    def _():
                        to_right(x_ref, p, ep, half).wait_send()

                    @pl.when(has_left)
                    def _():
                        to_left(x_ref, p, ep, half).wait_send()
                else:
                    chain_end(p, back, half)
    for step in range(1, total):
        note(me, step, lax.rem(me + step, total)).wait_send()
    own.wait()
    own_note.wait()


def gather_plane(tokens, note, nplane, nep, cut):
    rows, width = tokens.shape
    count = nplane * nep
    dma = pltpu.SemaphoreType.DMA
    vmem = pl.BlockSpec(memory_space=pltpu.VMEM)
    return pl.pallas_call(
        functools.partial(gather_kernel, nplane, nep, cut),
        out_shape=[
            jax.ShapeDtypeStruct((nplane, nep, rows, width), tokens.dtype),
            jax.ShapeDtypeStruct((2 * count,) + note.shape, note.dtype),
        ],
        in_specs=[vmem, vmem],
        out_specs=[vmem, vmem],
        scratch_shapes=[
            dma((2,)),
            dma((2 * (nplane - 1) * nep,)), dma((count,)), dma((nplane - 1,)), dma((count,)),
            dma((count,)), dma((count,)), dma((count,)), dma((count,)),
            dma((2 * count,)), dma((2 * count,)),
        ],
        compiler_params=pltpu.CompilerParams(collective_id=0, has_side_effects=True),
    )(tokens, note)


def scatter_kernel(
    nplane, nep, cut, part_ref, out_ref,
    land_a1, land_b1, mid_a, mid_b, land_a2, land_b2,
    send_a1, recv_a1, send_b1, recv_b1, send_a2, recv_a2, send_b2, recv_b2,
):
    plane, ep, plane_peer, ep_peer = place_of(nplane, nep)
    width = out_ref.shape[1]
    cols_a, cols_b = pl.ds(0, cut), pl.ds(cut, width - cut)
    greet(nplane, nep, plane_peer, ep_peer)

    def move(src, dst, send, recv, target):
        made = pltpu.make_async_remote_copy(
            src_ref=src, dst_ref=dst, send_sem=send, recv_sem=recv, device_id=target, device_id_type=MESH
        )
        made.start()
        return made

    first_a, first_b = {}, {}
    for item in range(1, max(nplane, nep) + 1):
        if item <= nep:
            e = lax.rem(ep + item, nep)
            for step in range(1, nplane):
                p, target = plane_peer(step)
                spot = (step - 1) * nep + item - 1
                first_a[item, step] = move(
                    part_ref.at[p, e, :, cols_a], land_a1.at[step - 1, item - 1],
                    send_a1.at[spot], recv_a1.at[spot], target,
                )
        if item <= nplane:
            p = lax.rem(plane + item, nplane)
            for step in range(1, nep):
                e, target = ep_peer(step)
                spot = (step - 1) * nplane + item - 1
                first_b[item, step] = move(
                    part_ref.at[p, e, :, cols_b], land_b1.at[step - 1, item - 1],
                    send_b1.at[spot], recv_b1.at[spot], target,
                )
    second_a, second_b = [], []
    for item in range(1, max(nplane, nep) + 1):
        if item <= nep:
            e, target = ep_peer(item)
            total = part_ref[plane, e, :, cols_a].astype(jnp.float32)
            for step in range(1, nplane):
                first_a[item, step].wait_recv()
                total = total + land_a1[step - 1, item - 1].astype(jnp.float32)
            if item < nep:
                mid_a[item - 1] = total.astype(mid_a.dtype)
                second_a.append(
                    move(mid_a.at[item - 1], land_a2.at[item - 1], send_a2.at[item - 1], recv_a2.at[item - 1], target)
                )
            else:
                total_a = total
        if item <= nplane:
            p, target = plane_peer(item)
            total = part_ref[p, ep, :, cols_b].astype(jnp.float32)
            for step in range(1, nep):
                first_b[item, step].wait_recv()
                total = total + land_b1[step - 1, item - 1].astype(jnp.float32)
            if item < nplane:
                mid_b[item - 1] = total.astype(mid_b.dtype)
                second_b.append(
                    move(mid_b.at[item - 1], land_b2.at[item - 1], send_b2.at[item - 1], recv_b2.at[item - 1], target)
                )
            else:
                total_b = total
    for index, made in enumerate(second_a):
        made.wait_recv()
        total_a = total_a + land_a2[index].astype(jnp.float32)
    out_ref[:, cols_a] = total_a.astype(out_ref.dtype)
    for index, made in enumerate(second_b):
        made.wait_recv()
        total_b = total_b + land_b2[index].astype(jnp.float32)
    out_ref[:, cols_b] = total_b.astype(out_ref.dtype)
    for made in list(first_a.values()) + list(first_b.values()) + second_a + second_b:
        made.wait_send()


def scatter_plane(parts, cut):
    nplane, nep, rows, width = parts.shape
    rest = width - cut
    kind = parts.dtype
    dma = pltpu.SemaphoreType.DMA
    pairs_a, pairs_b = (nplane - 1) * nep, (nep - 1) * nplane
    return pl.pallas_call(
        functools.partial(scatter_kernel, nplane, nep, cut),
        out_shape=jax.ShapeDtypeStruct((rows, width), kind),
        in_specs=[pl.BlockSpec(memory_space=pltpu.VMEM)],
        out_specs=pl.BlockSpec(memory_space=pltpu.VMEM),
        scratch_shapes=[
            pltpu.VMEM((nplane - 1, nep, rows, cut), kind),
            pltpu.VMEM((nep - 1, nplane, rows, rest), kind),
            pltpu.VMEM((nep - 1, rows, cut), kind),
            pltpu.VMEM((nplane - 1, rows, rest), kind),
            pltpu.VMEM((nep - 1, rows, cut), kind),
            pltpu.VMEM((nplane - 1, rows, rest), kind),
            dma((pairs_a,)), dma((pairs_a,)), dma((pairs_b,)), dma((pairs_b,)),
            dma((nep - 1,)), dma((nep - 1,)), dma((nplane - 1,)), dma((nplane - 1,)),
        ],
        compiler_params=pltpu.CompilerParams(collective_id=1, has_side_effects=True),
    )(parts)


def ring_spot(nplane, index):
    half = nplane // 2
    return lax.select(index < half, 2 * index, 2 * (nplane - 1 - index) + 1)


def ring_index(nplane, plane):
    row = lax.div(plane, 2)
    return lax.select(lax.rem(plane, 2) == 0, row, nplane - 1 - row)


def offsets(nep):
    return [0] + [side * back for back in range(1, nep) for side in (-1, 1)]


def gather_order(parts, nplane, nep):
    far = nplane // 2
    events, ready = [], 0.0
    for index, (kind, _, _, start) in enumerate(parts):
        events.append((start, 0, ("own", index, 0, 0, 0)))
        last = start
        if kind == "line":
            for off in offsets(nep):
                at = start + LINE_STEP * abs(off)
                if off:
                    events.append((at, 1, ("line", index, 0, off, 0)))
                for d in range(1, far + 1):
                    last = max(last, at + RING_STEP * d)
                    events.append((at + RING_STEP * d, 1 + d, ("ring", index, 0, off, d)))
        else:
            for d in range(1, far + 1):
                events.append((start + RING_STEP * d, 1 + d, ("ring", index, 0, 0, d)))
            for q in range(nplane):
                for off in offsets(nep)[1:]:
                    at = start + RING_STEP * min(q, nplane - q) + DEEP_STEP * abs(off)
                    last = max(last, at)
                    events.append((at, 2 + far, ("line", index, q, off, 0)))
        ready = last if index == 0 else max(last, ready)
        if index == 0:
            events.append((last, 3 + far, ("tables", index, 0, 0, 0)))
        for strip in range(parts[index][2] // STRIP):
            events.append((ready + PICK_STEP * strip, 4 + far, ("pick", index, strip, 0, 0)))
        for piece in range(PIECES):
            events.append((ready + PRODUCT_STEP * (piece + 1), 5 + far, ("product", index, piece, 0, 0)))
    events.sort()
    return [event for _, _, event in events]


def scatter_order(parts, nplane, nep):
    far = nplane // 2
    events = []
    for index, (kind, _, _, start) in enumerate(parts):
        events.append((start, 0, ("down", index, 0, 0, 0)))
        begin = start + SPREAD_STEP
        events.append((begin, 1, ("spread", index, 0, 0, 0)))
        if kind == "line":
            for off in offsets(nep):
                for d in range(far, -1, -1):
                    at = begin + BACK_RING * (far - d) + BACK_LINE * (nep - 1 - abs(off))
                    events.append((at, 2 + nep - abs(off), ("ring", index, 0, off, d)))
            at = begin + BACK_RING * far + BACK_LINE * (nep - 1) + BACK_LAST
            events.append((at, 3 + nep, ("last", index, 0, 0, 0)))
        else:
            for q in range(nplane):
                for off in offsets(nep):
                    at = begin + BACK_DEEP * (nep - 1 - abs(off))
                    events.append((at, 2 + nep - abs(off), ("line", index, q, off, 0)))
            done = begin + BACK_DEEP * (nep - 1)
            for d in range(far, -1, -1):
                events.append((done + BACK_RING * (far - d), 3 + nep, ("ring", index, 0, 0, d)))
    events.sort(key=lambda event: (event[0], event[1], event[2][1], event[2][2], -event[2][3], -event[2][4]))
    return [event for _, _, event in events]


def layer_kernel(
    plan, hot_hbm, tok_ref, ids_hbm, picks_hbm, gates_hbm, wg_hbm, wu_hbm, wd_hbm, out_ref, load_ref,
    hot_ref, ids_ref, picks_ref, gates_ref, xs, sel, back, wg, wu, wd, inputs, stage, acc_g, acc_u, hidden, pairs, stage2, parts_ref,
    ring_land, line_land, deep_land, count_own, count_in,
    own_sem, small_sem, w_sem, pool_ring, pool_line, x_ring, x_line, swap_send, swap_recv, ring_recv, line_recv, deep_recv,
):
    nplane, nep, most, into, outof = plan
    far = nplane // 2
    count = nplane * nep
    rows, width = out_ref.shape
    top = ids_ref.shape[0]
    total = count * rows
    cap = stage.shape[0]
    ngroup = 2 * nplane
    group = lax.axis_index("group")
    ep = lax.axis_index("ep")
    core = lax.rem(group, 2)
    me_ring = ring_index(nplane, lax.div(group, 2))
    partner_group = group + 1 - 2 * core
    partner = (partner_group, ep)
    f32 = jnp.float32
    bf16 = jnp.bfloat16

    def spot(q):
        return lax.rem(me_ring + q + nplane, nplane)

    def ring_peer(side):
        return (ring_spot(nplane, spot(side)) * 2 + core, ep)

    peers = {1: ring_peer(1), -1: ring_peer(-1)}
    line_peers = {1: (group, lax.min(ep + 1, nep - 1)), -1: (group, lax.max(ep - 1, 0))}
    has = {1: ep < nep - 1, -1: ep > 0}

    def valid(off):
        if off == 0:
            return None
        return (ep + off < nep) if off > 0 else (ep + off >= 0)

    def both(a, b):
        if a is None:
            return b
        return a if b is None else a & b

    def when(cond, run):
        if cond is None:
            run()
        else:
            pl.when(cond)(run)

    pools = {key: [] for key in (("ring", 1), ("ring", -1), ("line", 1), ("line", -1))}
    swaps = []

    def copy(src, dst, send, recv, target):
        return pltpu.make_async_remote_copy(
            src_ref=src, dst_ref=dst, send_sem=send, recv_sem=recv, device_id=target, device_id_type=MESH
        )

    def send_out(cond, kind, side, make):
        pool = pools[kind, side]
        sems = (pool_ring if kind == "ring" else pool_line).at[0 if side > 0 else 1]
        turn = len(pool) % sems.shape[0]
        if len(pool) >= sems.shape[0]:
            old_cond, old = pool[-sems.shape[0]]
            when(old_cond, lambda: old().wait_send())

        def ready():
            return make(sems.at[turn])

        when(cond, lambda: ready().start())
        pool.append((cond, ready))

    def swap(make):
        make().start()
        swaps.append(make)

    lead = xs.shape[2] - width
    own_block = me_ring * nep + ep
    small_copies = []
    for index, (src, dst) in enumerate(
        ((ids_hbm, ids_ref), (picks_hbm, picks_ref), (gates_hbm, gates_ref), (hot_hbm, hot_ref))
    ):
        made = pltpu.make_async_copy(src, dst, small_sem.at[index])
        made.start()
        small_copies.append(made)
    own_copies = []
    for index, (_, c0, cols, _) in enumerate(into):
        made = pltpu.make_async_copy(
            tok_ref.at[:, pl.ds(c0, cols)], xs.at[own_block, :, pl.ds(lead + c0, cols)], own_sem.at[index]
        )
        made.start()
        own_copies.append(made)
    weight_copies = []
    for index, (src, dst) in enumerate(((wg_hbm, wg), (wu_hbm, wu), (wd_hbm, wd))):
        made = pltpu.make_async_copy(src, dst, w_sem.at[index])
        made.start()
        weight_copies.append(made)

    barrier = pltpu.get_barrier_semaphore()
    for target in (partner, peers[1], peers[-1]):
        pl.semaphore_signal(barrier, inc=1, device_id=target, device_id_type=MESH)
    for side in (1, -1):
        @pl.when(has[side])
        def _(side=side):
            pl.semaphore_signal(barrier, inc=1, device_id=line_peers[side], device_id_type=MESH)

    for made in small_copies:
        made.wait()
    own = jnp.concatenate(
        [ids_ref[...].astype(f32), picks_ref[...].astype(f32), gates_ref[...]], axis=0
    )
    own = jnp.concatenate([own, jnp.zeros((3 * top, lead - rows), f32)], axis=1)
    own = jnp.concatenate([own, jnp.zeros((lead - 3 * top, lead), f32)], axis=0)
    xs[own_block, :, pl.ds(0, lead)] = own.T[:rows].astype(bf16)
    pl.semaphore_wait(barrier, 3 + has[1].astype(jnp.int32) + has[-1].astype(jnp.int32))

    def span_of(index):
        _, c0, cols, _ = into[index]
        return (0, lead + cols) if c0 == 0 else (lead + c0, cols)

    def x_launch(cond, sem, kind, side, block, cols, target):
        part = xs.at[block, :, pl.ds(cols[0], cols[1])]
        send_out(cond, kind, side, lambda send: copy(part, part, send, sem, target))

    def x_wait(sem, blocks, cols):
        part = xs.at[pl.ds(0, blocks), :, pl.ds(cols[0], cols[1])]
        copy(part, part, pool_ring.at[0, 0], sem, partner).wait_recv()

    def halves(c0, cols):
        low = cols // 256 * 128
        return {1: (c0, low), -1: (c0 + low, cols - low)}

    starts_x = [0]
    for kind, _, _, _ in into:
        starts_x.append(starts_x[-1] + (nep if kind == "line" else count))

    def line_sem(index, q, off):
        at = starts_x[index] + ep + off
        return x_line.at[at if into[index][0] == "line" else at + spot(q) * nep]

    def ring_out(cond, index, block, off, side, d):
        span = span_of(index) if d < far else halves(*span_of(index))[side]
        x_launch(cond, x_ring.at[index, d - 1, ep + off], "ring", side, block, span, peers[side])

    def line_out(index, q, off, side):
        cond = both(valid(off), has[side])
        block = spot(q) * nep + ep + off
        x_launch(cond, line_sem(index, q, off), "line", side, block, span_of(index), line_peers[side])

    def gather_own(index):
        own_copies[index].wait()
        for side in (1, -1):
            line_out(index, 0, 0, side)
        for side in (1, -1):
            ring_out(None, index, own_block, 0, side, 1)

    def gather_line(index, q, off):
        block = spot(q) * nep + ep + off
        when(valid(off), lambda: x_wait(line_sem(index, q, off), 1, span_of(index)))
        line_out(index, q, off, 1 if off < 0 else -1)
        if into[index][0] == "line":
            for side in (1, -1):
                ring_out(valid(off), index, block, off, side, 1)

    def gather_ring(index, off, d):
        sem = x_ring.at[index, d - 1, ep + off]
        when(valid(off), lambda: x_wait(sem, 2 if d < far else 1, span_of(index)))
        for side in (1, -1):
            if d < far:
                block = spot(-side * d) * nep + ep + off
                ring_out(valid(off), index, block, off, side, d + 1)
                if into[index][0] == "ring":
                    for way in (1, -1):
                        line_out(index, -side * d, 0, way)
        if d == far and into[index][0] == "ring":
            for way in (1, -1):
                line_out(index, far, 0, way)

    def tables():
        expert = group * nep + ep
        other = partner_group * nep + ep
        hot = (hot_ref[ep] * nep + ep).astype(f32)
        expert_f, other_f = expert.astype(f32), other.astype(f32)
        block_rows = rows // 2
        a = lax.broadcasted_iota(jnp.int32, (128, 128), 0)
        b = lax.broadcasted_iota(jnp.int32, (128, 128), 1)
        before = ((lax.div(a, block_rows) == lax.div(b, block_rows)) & (a < b)).astype(f32)
        sub = lax.broadcasted_iota(jnp.int32, (8, 128), 0)
        lane8 = lax.broadcasted_iota(jnp.int32, (8, 128), 1)
        slot = lax.broadcasted_iota(jnp.int32, (cap, 128), 0).astype(f32)
        sums = [jnp.zeros((1, 1), f32) for _ in range(4)]

        def add_up(flag):
            return jnp.sum(jnp.sum(flag.astype(f32), axis=1, keepdims=True), axis=0, keepdims=True)

        for chunk in range(total // 128):
            at = pl.ds(chunk * 128, 128)
            fit = 128 // rows
            tile = xs[pl.ds(chunk * fit, fit), :, pl.ds(0, lead)].reshape(128, lead).astype(f32).T
            ids, picks, gates = tile[:top], tile[top:2 * top], tile[2 * top:3 * top]
            chosen = [ids == expert_f, ids == other_f]
            flag = [jnp.sum(c.astype(f32), axis=0, keepdims=True) for c in chosen]
            scale = [jnp.sum(jnp.where(c, gates, 0.0), axis=0, keepdims=True) for c in chosen]
            stacked = jnp.where(sub == 0, flag[0], jnp.where(sub == 1, flag[1], 0.0))
            rank = jnp.dot(stacked, before, preferred_element_type=f32)
            first = (lax.div(lane8[0:1], block_rows) + chunk * (128 // block_rows)).astype(f32) * most
            scaled = []
            for which in range(2):
                position = jnp.where(flag[which] > 0, first + rank[which:which + 1], -1.0)
                one = (slot == position).astype(f32)
                sel[pl.ds(which * cap, cap), at] = one.astype(bf16)
                scaled.append(one * scale[which])
            back[at, :] = jnp.concatenate(scaled, axis=0).T.astype(bf16)
            copied = (ids == hot) & (picks < ngroup)
            for which, (here, its) in enumerate(((expert_f, group), (other_f, partner_group))):
                sums[2 * which] = sums[2 * which] + add_up((ids == here) & ~copied)
                sums[2 * which + 1] = sums[2 * which + 1] + add_up(copied & (picks == its.astype(f32)))
        lane_n = lane8
        count_own[0] = jnp.where(lane_n == 0, sums[0], jnp.where(lane_n == 1, sums[1], 0.0))
        count_own[1] = jnp.where(lane_n == 0, sums[2], jnp.where(lane_n == 1, sums[3], 0.0))
        swap(count_copy)

    def count_copy():
        spare = len(into) + len(outof)
        return copy(count_own.at[1], count_in, swap_send.at[spare], swap_recv.at[spare], partner)

    step = 256

    def in_copy(index):
        _, c0, cols, _ = into[index]
        return copy(
            stage.at[:, pl.ds(c0, cols)], inputs.at[pl.ds(cap, cap), pl.ds(c0, cols)],
            swap_send.at[index], swap_recv.at[index], partner,
        )

    def pick(index, strip):
        _, c0, cols, _ = into[index]

        at, here = pl.ds(c0 + strip * STRIP, STRIP), pl.ds(lead + c0 + strip * STRIP, STRIP)
        got = jnp.dot(sel[...], xs[:, :, here].reshape(total, STRIP), preferred_element_type=f32).astype(bf16)
        inputs[pl.ds(0, cap), at] = got[:cap]
        stage[:, at] = got[cap:]
        if strip == cols // STRIP - 1:
            swap(lambda: in_copy(index))

    seen = []

    def product(index, piece):
        _, c0, cols, _ = into[index]
        if piece == 0:
            in_copy(index).wait_recv()
            if not seen:
                weight_copies[0].wait()
                weight_copies[1].wait()
        first = piece not in seen
        seen.append(piece)
        last = seen.count(piece) == len(into)
        tiles = acc_g.shape[1] // step // PIECES

        def part(j, _):
            at = pl.ds(pl.multiple_of((piece * tiles + j) * step, step), step)
            acts = []
            for weight, acc in ((wg, acc_g), (wu, acc_u)):
                got = jnp.dot(
                    inputs[:, pl.ds(c0, cols)], weight[pl.ds(c0, cols), at], preferred_element_type=f32
                )
                acts.append(got if first else acc[:, at] + got)
            if last:
                hidden[:, at] = (acts[0] / (1.0 + jnp.exp(-acts[0])) * acts[1]).astype(bf16)
            else:
                acc_g[:, at], acc_u[:, at] = acts
            return 0

        lax.fori_loop(0, tiles, part, 0)

    def back_copy(index):
        _, c0, cols, _ = outof[index]
        spot_of = len(into) + index
        return copy(
            stage2.at[:, pl.ds(c0, cols)], pairs.at[pl.ds(cap, cap), pl.ds(c0, cols)],
            swap_send.at[spot_of], swap_recv.at[spot_of], partner,
        )

    def down(index):
        _, c0, cols, _ = outof[index]

        def part(i, _):
            at = pl.ds(pl.multiple_of(c0 + i * step, step), step)
            got = jnp.dot(hidden[...], wd[:, at], preferred_element_type=f32).astype(bf16)
            pairs[pl.ds(0, cap), at] = got[:cap]
            stage2[:, at] = got[cap:]
            return 0

        lax.fori_loop(0, cols // step, part, 0)
        swap(lambda: back_copy(index))

    def spread(index):
        _, c0, cols, _ = outof[index]
        back_copy(index).wait_recv()

        def part(i, _):
            at = pl.ds(pl.multiple_of(c0 + i * step, step), step)
            got = jnp.dot(back[...], pairs[:, at], preferred_element_type=f32).astype(bf16)
            parts_ref[:, :, at] = got.reshape(count, rows, step)
            return 0

        lax.fori_loop(0, cols // step, part, 0)

    def add(dst, sources):
        def part(i, _):
            at = pl.ds(pl.multiple_of(i * 16, 16), 16)
            value = sources[0][at, :].astype(f32)
            for source in sources[1:]:
                value = value + source[at, :].astype(f32)
            dst[at, :] = value.astype(dst.dtype)
            return 0

        lax.fori_loop(0, rows // 16, part, 0)

    def way(side):
        return 0 if side > 0 else 1

    starts_r = [0]
    for kind, _, _, _ in outof:
        starts_r.append(starts_r[-1] + (nep if kind == "line" else 1))

    def ring_sem(index, d, off):
        return ring_recv.at[starts_r[index] + (ep + off if outof[index][0] == "line" else 0), d]

    def ring_slot(side, d, off, span):
        return ring_land.at[way(side), d, ep + off, :, pl.ds(span[0], span[1])]

    def ring_send(cond, index, off, side, d, span):
        dst = ring_slot(side, d - 1, off, span)
        src = block(side * d, off, span)
        send_out(
            cond, "ring", side, lambda send: copy(src, dst, send, ring_sem(index, d - 1, off), peers[side])
        )

    def ring_await(index, off, d, blocks):
        _, c0, cols, _ = outof[index]
        part = ring_land.at[0, 0, pl.ds(0, blocks), :, pl.ds(c0, cols)]
        copy(part, part, pool_ring.at[0, 0], ring_sem(index, d, off), partner).wait_recv()

    def deep_slot(side, q, off, span):
        return deep_land.at[way(side), spot(q) * nep + ep + off, :, pl.ds(span[0], span[1])]

    def deep_sem(index, side, q, off):
        return deep_recv.at[deep_of[index], way(side), spot(q) * nep + ep + off]

    deep_of, lined = {}, {}
    for index, (kind, _, _, _) in enumerate(outof):
        if kind == "line":
            lined[index] = len(lined)
        else:
            deep_of[index] = len(deep_of)

    def deep_send(cond, index, q, off, side):
        _, c0, cols, _ = outof[index]
        src, dst = block(q, off, (c0, cols)), deep_slot(side, q, off, (c0, cols))
        send_out(
            cond, "line", side, lambda send: copy(src, dst, send, deep_sem(index, side, q, off), line_peers[side])
        )

    def deep_await(index, side, q, off):
        _, c0, cols, _ = outof[index]
        part = deep_slot(side, q, off, (c0, cols))
        copy(part, part, pool_ring.at[0, 0], deep_sem(index, side, q, off), partner).wait_recv()
        return part

    def line_direct(index, off):
        _, c0, cols, _ = outof[index]
        src, dst = block(0, off, (c0, cols)), line_land.at[ep, :, pl.ds(c0, cols)]
        sem = line_recv.at[lined[index]]
        side = 1 if off > 0 else -1
        send_out(valid(off), "line", side, lambda send: copy(src, dst, send, sem, (group, ep + off)))

    def block(q, off, span):
        return parts_ref.at[spot(q) * nep + ep + off, :, pl.ds(span[0], span[1])]

    def scatter_line(index, q, off):
        _, c0, cols, _ = outof[index]
        here = block(q, off, (c0, cols))
        if off != 0:
            side = 1 if off > 0 else -1
            behind = has[-side]

            @pl.when(both(valid(off), behind))
            def _():
                add(here, [here, deep_await(index, side, q, off)])

            deep_send(valid(off), index, q, off, side)
        else:
            left, right = has[-1], has[1]

            @pl.when(left & right)
            def _():
                add(here, [here, deep_await(index, 1, q, 0), deep_await(index, -1, q, 0)])

            @pl.when(left & jnp.logical_not(right))
            def _():
                add(here, [here, deep_await(index, 1, q, 0)])

            @pl.when(right & jnp.logical_not(left))
            def _():
                add(here, [here, deep_await(index, -1, q, 0)])

    def plane_terms(off, span):
        return [block(0, off, span)] + [ring_slot(side, 0, off, span) for side in (1, -1)]

    def scatter_ring(index, off, d):
        kind, c0, cols, _ = outof[index]
        whole = (c0, cols)
        split = halves(c0, cols)
        if d == far:
            for side in (1, -1):
                ring_send(valid(off), index, off, side, d, split[side])
            if far > 1:
                for side in (1, -1):
                    ring_send(valid(off), index, off, side, d - 1, split[-side])
        elif d > 0:
            when(valid(off), lambda: ring_await(index, off, d, 1 if d + 1 == far else 2))
            for side in (1, -1):
                for span in [split[side]] if d + 1 == far else [whole]:
                    def go(side=side, span=span):
                        here = block(side * d, off, span)
                        add(here, [here, ring_slot(side, d, off, span)])

                    when(valid(off), go)
                    ring_send(valid(off), index, off, side, d, span)
        else:
            when(valid(off), lambda: ring_await(index, off, 0, 1 if far == 1 else 2))
            if off != 0:
                when(valid(off), lambda: add(block(0, off, whole), plane_terms(off, whole)))
                line_direct(index, off)
            elif kind == "ring":
                add(out_ref.at[:, pl.ds(c0, cols)], plane_terms(0, whole))

    def scatter_last(index):
        _, c0, cols, _ = outof[index]
        at = pl.ds(c0, cols)
        part = line_land.at[pl.ds(0, nep - 1), :, at]
        copy(part, part, pool_line.at[0, 0], line_recv.at[lined[index]], partner).wait_recv()
        others = [line_land.at[lax.rem(ep + step, nep), :, at] for step in range(1, nep)]
        add(out_ref.at[:, at], plane_terms(0, (c0, cols)) + others)

    for what, index, q, off, d in gather_order(into, nplane, nep):
        if what == "tables":
            tables()
        elif what == "own":
            gather_own(index)
        elif what == "line":
            gather_line(index, q, off)
        elif what == "ring":
            gather_ring(index, off, d)
        elif what == "pick":
            pick(index, q)
        else:
            product(index, q)
    weight_copies[2].wait()
    for what, index, q, off, d in scatter_order(outof, nplane, nep):
        if what == "down":
            down(index)
        elif what == "spread":
            spread(index)
        elif what == "ring":
            scatter_ring(index, off, d)
        elif what == "last":
            scatter_last(index)
        else:
            scatter_line(index, q, off)
    count_copy().wait_recv()
    load_ref[...] = (count_own[0] + count_in[...])[0:1, 0:2] / top
    for make in swaps:
        make().wait_send()
    for (kind, _), pool in pools.items():
        for cond, make in pool[-(pool_ring if kind == "ring" else pool_line).shape[1]:]:
            when(cond, lambda: make().wait_send())

def finish_kernel(mixed_in, load_in, mixed_out, load_out, mixed_here, load_here, sems):
    trips = ((mixed_in, mixed_here, mixed_out), (load_in, load_here, load_out))
    for way in range(2):
        made = []
        for index, trip in enumerate(trips):
            made.append(pltpu.make_async_copy(trip[way], trip[way + 1], sems.at[way, index]))
            made[-1].start()
        for one in made:
            one.wait()


def layer(tokens, ids, picks, gates, hot, w_gate, w_up, w_down, plan, shapes, need):
    nplane, nep, _, into, outof = plan
    far = nplane // 2
    count = nplane * nep
    rows, width = tokens.shape
    dma = pltpu.SemaphoreType.DMA
    vmem = pl.BlockSpec(memory_space=pltpu.VMEM)
    hbm = pl.BlockSpec(memory_space=pltpu.HBM)
    lines_in = sum(kind == "line" for kind, _, _, _ in into)
    lines_out = sum(kind == "line" for kind, _, _, _ in outof)
    rings_in, rings_out = len(into) - lines_in, len(outof) - lines_out
    swaps = len(into) + len(outof) + 1
    mixed, loads = pl.pallas_call(
        functools.partial(layer_kernel, plan),
        out_shape=[
            jax.ShapeDtypeStruct((rows, width), tokens.dtype),
            jax.ShapeDtypeStruct((1, 2), jnp.float32),
        ],
        in_specs=[hbm] * 8,
        out_specs=[vmem, vmem],
        scratch_shapes=[pltpu.SMEM(hot.shape, hot.dtype)] + [
            pltpu.VMEM(x.shape, x.dtype) for x in (ids, picks, gates)
        ] + [pltpu.VMEM(shape, kind) for shape, kind in shapes] + [
            dma((len(into),)), dma((4,)), dma((3,)), dma((2, POOL)), dma((2, POOL)),
            dma((len(into), far, nep)), dma((lines_in * nep + rings_in * count,)), dma((swaps,)), dma((swaps,)),
            dma((lines_out * nep + rings_out, far)), dma((lines_out,)), dma((rings_out, 2, count)),
        ],
        compiler_params=pltpu.CompilerParams(
            collective_id=2, has_side_effects=True, vmem_limit_bytes=VMEM_LIMIT
        ),
    )(hot, tokens, ids, picks, gates, w_gate, w_up, w_down)
    return pl.pallas_call(
        finish_kernel,
        out_shape=[jax.ShapeDtypeStruct(x.shape, x.dtype) for x in (mixed, loads)],
        in_specs=[hbm, hbm],
        out_specs=[hbm, hbm],
        scratch_shapes=[pltpu.VMEM(x.shape, x.dtype) for x in (mixed, loads)] + [dma((2, 2))],
        compiler_params=pltpu.CompilerParams(vmem_limit_bytes=VMEM_LIMIT),
    )(mixed, loads)


def buffers(nplane, nep, rows, width, top, hidden, cap, kind):
    count = nplane * nep
    total = count * rows
    f32 = jnp.float32
    return [
        ((count, rows, width + 128), kind),
        ((2 * cap, total), kind), ((total, 2 * cap), kind),
        ((width, hidden), kind), ((width, hidden), kind), ((hidden, width), kind),
        ((2 * cap, width), kind), ((cap, width), kind),
        ((2 * cap, hidden), f32), ((2 * cap, hidden), f32), ((2 * cap, hidden), kind),
        ((2 * cap, width), kind), ((cap, width), kind), ((count, rows, width), kind),
        ((2, nplane // 2, nep, rows, width), kind), ((nep, rows, width), kind),
        ((2, count, rows, width), kind),
        ((2, 8, 128), f32), ((8, 128), f32),
    ]


def cuts(width, shares):
    unit = 256
    units = width // unit
    total = sum(share for _, share, _ in shares)
    made, at, seen = [], 0, 0
    for kind, share, start in shares:
        seen += share
        end = units * seen // total
        made.append((kind, at * unit, (end - at) * unit, start))
        at = end
    return tuple(made)


def body(
    tokens, expert_ids, gate_scores, replica_pick, replica_hot, gate_weight, up_weight, down_weight
):
    ngroup = lax.axis_size("group")
    nep = lax.axis_size("ep")
    nplane = ngroup // 2
    device_count = ngroup * nep
    group_index = lax.axis_index("group")
    ep_index = lax.axis_index("ep")
    core = group_index % 2
    me = group_index * nep + ep_index
    partner = (group_index + 1 - 2 * core) * nep + ep_index
    tok_dev, width = tokens.shape
    top_count = expert_ids.shape[1]
    most = (tok_dev // 2 * top_count + device_count - 1) // device_count + 1
    capacity = 2 * most * nplane * nep
    cut = width // 256 * 128
    back_cut = width * 11 // 14 // 128 * 128

    hidden = gate_weight.shape[2]
    plan_shapes = buffers(nplane, nep, tok_dev, width, top_count, hidden, capacity, tokens.dtype)
    need = sum(math.prod(shape) * jnp.dtype(kind).itemsize for shape, kind in plan_shapes)
    if nplane % 2 == 0 and nplane > 2 and device_count <= 256 and need < VMEM_LIMIT * 7 // 8:
        plan = (nplane, nep, most, cuts(width, INTO), cuts(width, OUTOF))
        return layer(
            tokens, expert_ids.T, replica_pick.T, gate_scores.T, replica_hot,
            gate_weight[0], up_weight[0], down_weight[0], plan, plan_shapes, need,
        )

    coded = expert_ids * (ngroup + 1) + replica_pick
    note = jnp.concatenate([coded.astype(jnp.float32), gate_scores], axis=1).reshape(-1, 128)
    every, notes = gather_plane(tokens, note, nplane, nep, cut)
    every = every.reshape(nplane * nep * tok_dev, width)
    routing = notes.reshape(device_count * tok_dev, 2 * top_count)
    coded = routing[:, :top_count].astype(jnp.int32)
    ids = coded // (ngroup + 1)
    picks = coded % (ngroup + 1)
    hot = replica_hot[ep_index]
    replicated = (ids % nep == ep_index) & (ids // nep == hot) & (picks < ngroup)
    primary_load = jnp.sum(((ids == me) & ~replicated).astype(jnp.float32))
    replica_load = jnp.sum((replicated & (picks == group_index)).astype(jnp.float32))
    loads = jnp.stack([primary_load, replica_load])[None, :] / top_count

    mine = routing.reshape(nplane, 2, nep * tok_dev, 2 * top_count)
    mine = lax.dynamic_index_in_dim(mine, core, 1, keepdims=False).reshape(-1, 2 * top_count)
    my_ids = mine[:, :top_count].astype(jnp.int32) // (ngroup + 1)
    my_gates = mine[:, top_count:]

    def spots(expert):
        chosen = my_ids == expert
        mask = jnp.any(chosen, axis=1)
        scale = jnp.sum(jnp.where(chosen, my_gates, 0.0), axis=1)
        place = jnp.where(mask, jnp.cumsum(mask.astype(jnp.int32)) - 1, -1)
        spot = place[None, :] == jnp.arange(capacity, dtype=jnp.int32)[:, None]
        return spot, jnp.sum(jnp.where(spot, scale[None, :], 0.0), axis=1)

    spot_me, scale_me = spots(me)
    spot_other, scale_other = spots(partner)
    select = jnp.concatenate([spot_me, spot_other], axis=0).astype(jnp.bfloat16)
    row_scale = jnp.concatenate([scale_me, scale_other], axis=0)
    swap = [(index, index ^ 1) for index in range(ngroup)]

    picked = jnp.dot(select, every, preferred_element_type=jnp.float32).astype(jnp.bfloat16)
    inputs = jnp.concatenate(
        [picked[:capacity], lax.ppermute(picked[capacity:], "group", swap)], axis=0
    )
    gate_act = jnp.dot(inputs, gate_weight[0], preferred_element_type=jnp.float32)
    up_act = jnp.dot(inputs, up_weight[0], preferred_element_type=jnp.float32)
    hidden = (jax.nn.silu(gate_act) * up_act).astype(jnp.bfloat16)
    pair_out = jnp.dot(hidden, down_weight[0], preferred_element_type=jnp.float32).astype(jnp.bfloat16)
    pairs = jnp.concatenate(
        [pair_out[:capacity], lax.ppermute(pair_out[capacity:], "group", swap)], axis=0
    )
    scaled = (pairs.astype(jnp.float32) * row_scale[:, None]).astype(jnp.bfloat16)
    spread = lax.dot_general(
        select, scaled, (((0,), (0,)), ((), ())), preferred_element_type=jnp.float32
    ).astype(jnp.bfloat16)
    mixed = scatter_plane(spread.reshape(nplane, nep, tok_dev, width), back_cut)
    return mixed, loads


def solution(mesh):
    rows = P(AXES, None)
    weights = P(AXES, None, None)
    return jax.shard_map(
        body,
        mesh=mesh,
        in_specs=(rows, rows, rows, rows, P(), weights, weights, weights),
        out_specs=(rows, rows),
        check_vma=False,
    )
```
